8 devices in a mesh: dp: 1 (over z), ei: 2 (over y), eo: 4 (over x, core).
Axes of the slice: x: 2, y: 2, z: 1, core: 2. Of those that a mesh axis runs over, the one named last changes fastest.
Arguments:
- tokens: bfloat16 [512, 2048], P(('dp', 'ei', 'eo'))
- expert_idx: int32 [512, 6], P(('dp', 'ei', 'eo'))
- gates: float32 [512, 6], P(('dp', 'ei', 'eo'))
- w_gate: bfloat16 [32, 2048, 1408], P(('ei', 'eo'))
- w_up: bfloat16 [32, 2048, 1408], P(('ei', 'eo'))
- w_down: bfloat16 [32, 1408, 2048], P(('ei', 'eo'))
- grad_out: bfloat16 [512, 2048], P(('dp', 'ei', 'eo'))
Outputs:
- output 1: bfloat16 [512, 2048], P(('dp', 'ei', 'eo'))
- output 2: bfloat16 [512, 2048], P(('dp', 'ei', 'eo'))
- output 3: float32 [512, 6], P(('dp', 'ei', 'eo'))
- output 4: bfloat16 [32, 2048, 1408], P(('dp', 'ei', 'eo'))
- output 5: bfloat16 [32, 2048, 1408], P(('dp', 'ei', 'eo'))
- output 6: bfloat16 [32, 1408, 2048], P(('dp', 'ei', 'eo'))
All inputs are finite; a program needn't handle non-finite values.
Results may differ from the reference program's by a relative error of at most 0.00167.
Values are sent between devices in bfloat16 or wider.
A program may use at most 1 GiB of HBM per device.

```python
import jax
import jax.numpy as jnp
from jax import lax

GROUP_DEVS = 8
EXP_DEV = 4
TOK_DEV = 64
D_MODEL = 2048
D_FF = 1408
TOP_K = 6
NUM_EXPERTS = EXP_DEV * GROUP_DEVS
TOKENS = TOK_DEV * GROUP_DEVS
CAPACITY = min(TOK_DEV, TOK_DEV * TOP_K // (4 * EXP_DEV))


def draw_routes(route_key):
    hot_key, src_key = jax.random.split(route_key)
    hot_dev = jax.random.randint(hot_key, (), 0, GROUP_DEVS)
    expert_ids = jnp.arange(NUM_EXPERTS, dtype=jnp.int32)
    is_hot = expert_ids // EXP_DEV == hot_dev
    cold_n = NUM_EXPERTS - EXP_DEV
    rest_n = TOK_DEV * TOP_K - EXP_DEV * CAPACITY
    above_hot = (expert_ids >= (hot_dev + 1) * EXP_DEV).astype(jnp.int32)
    cold_pos = jnp.clip(expert_ids - EXP_DEV * above_hot, 0, cold_n - 1)
    positions = jnp.arange(TOK_DEV * TOP_K, dtype=jnp.int32)

    def one_source(source_key):
        perm_key, row_key, rot_key = jax.random.split(source_key, 3)
        cold_rank = jax.random.permutation(perm_key, cold_n)
        cold_count = rest_n // cold_n + (cold_rank[cold_pos] < rest_n % cold_n).astype(jnp.int32)
        counts = jnp.where(is_hot, CAPACITY, cold_count).astype(jnp.int32)
        listing = jnp.searchsorted(jnp.cumsum(counts), positions, side='right').astype(jnp.int32)
        route_table = listing.reshape(TOP_K, TOK_DEV).T[jax.random.permutation(row_key, TOK_DEV)]
        row_shift = jax.random.randint(rot_key, (TOK_DEV, 1), 0, TOP_K)
        col_order = (jnp.arange(TOP_K)[None, :] + row_shift) % TOP_K
        return jnp.take_along_axis(route_table, col_order, axis=1)

    source_keys = jax.random.split(src_key, GROUP_DEVS)
    return jax.vmap(one_source)(source_keys).reshape(TOKENS, TOP_K).astype(jnp.int32)


def setup_inputs(seed: int = 0, part: int = 0) -> dict:
    part_key = jax.random.fold_in(jax.random.key(seed), part)
    tok_key, route_key, gate_key, dy_key = jax.random.split(part_key, 4)
    gate_w_key, up_w_key, down_w_key = jax.random.split(jax.random.key(seed + 1), 3)
    tokens = jax.random.normal(tok_key, (TOKENS, D_MODEL), jnp.float32).astype(jnp.bfloat16)
    expert_idx = draw_routes(route_key)
    gates = jax.random.uniform(gate_key, (TOKENS, TOP_K), jnp.float32, 0.05, 0.3)
    w_gate = (jax.random.normal(gate_w_key, (NUM_EXPERTS, D_MODEL, D_FF), jnp.float32) * D_MODEL ** -0.5).astype(jnp.bfloat16)
    w_up = (jax.random.normal(up_w_key, (NUM_EXPERTS, D_MODEL, D_FF), jnp.float32) * D_MODEL ** -0.5).astype(jnp.bfloat16)
    w_down = (jax.random.normal(down_w_key, (NUM_EXPERTS, D_FF, D_MODEL), jnp.float32) * D_FF ** -0.5).astype(jnp.bfloat16)
    grad_out = jax.random.normal(dy_key, (TOKENS, D_MODEL), jnp.float32).astype(jnp.bfloat16)
    return {'tokens': tokens, 'expert_idx': expert_idx, 'gates': gates, 'w_gate': w_gate, 'w_up': w_up, 'w_down': w_down, 'grad_out': grad_out}


def reference(tokens, expert_idx, gates, w_gate, w_up, w_down, grad_out):
    n_assign = TOKENS * TOP_K
    expert_cap = GROUP_DEVS * CAPACITY
    flat_e = expert_idx.reshape(-1)
    sort_order = jnp.argsort(flat_e, stable=True).astype(jnp.int32)
    sorted_e = flat_e[sort_order]
    counts = jnp.zeros((NUM_EXPERTS,), jnp.int32).at[flat_e].add(1)
    starts = jnp.cumsum(counts) - counts
    slot_rank = jnp.arange(n_assign, dtype=jnp.int32) - starts[sorted_e]
    filler = jnp.full((NUM_EXPERTS * expert_cap,), n_assign, jnp.int32).at[sorted_e * expert_cap + slot_rank].set(sort_order)
    filler = filler.reshape(NUM_EXPERTS, expert_cap)
    tok_pad = jnp.concatenate([tokens, jnp.zeros((1, D_MODEL), tokens.dtype)])
    dy_pad = jnp.concatenate([grad_out, jnp.zeros((1, D_MODEL), grad_out.dtype)])
    gate_pad = jnp.concatenate([gates.reshape(-1), jnp.zeros((1,), jnp.float32)])

    def one_expert(acc_state, expert_in):
        out_acc, dx_acc, dg_acc = acc_state
        wg_e, wu_e, wd_e, assign = expert_in
        tok_ids = assign // TOP_K
        x_rows = tok_pad[tok_ids]
        g_rows = gate_pad[assign]
        dy_rows = dy_pad[tok_ids]
        h_gate = jnp.dot(x_rows, wg_e, preferred_element_type=jnp.float32)
        h_up = jnp.dot(x_rows, wu_e, preferred_element_type=jnp.float32)
        sig_gate = jax.nn.sigmoid(h_gate)
        hidden = (h_gate * sig_gate * h_up).astype(jnp.bfloat16)
        y_rows = jnp.dot(hidden, wd_e, preferred_element_type=jnp.float32).astype(jnp.bfloat16)
        dg_rows = jnp.sum(dy_rows.astype(jnp.float32) * y_rows.astype(jnp.float32), axis=1)
        u_rows = (g_rows[:, None] * dy_rows.astype(jnp.float32)).astype(jnp.bfloat16)
        d_hidden = jnp.dot(u_rows, wd_e.T, preferred_element_type=jnp.float32)
        d_up = (d_hidden * h_gate * sig_gate).astype(jnp.bfloat16)
        d_gate = (d_hidden * h_up * sig_gate * (1.0 + h_gate * (1.0 - sig_gate))).astype(jnp.bfloat16)
        dx_rows = (jnp.dot(d_gate, wg_e.T, preferred_element_type=jnp.float32) + jnp.dot(d_up, wu_e.T, preferred_element_type=jnp.float32)).astype(jnp.bfloat16)
        dw_gate = jnp.dot(x_rows.T, d_gate, preferred_element_type=jnp.float32).astype(jnp.bfloat16)
        dw_up = jnp.dot(x_rows.T, d_up, preferred_element_type=jnp.float32).astype(jnp.bfloat16)
        dw_down = jnp.dot(hidden.T, u_rows, preferred_element_type=jnp.float32).astype(jnp.bfloat16)
        out_acc = out_acc.at[tok_ids].add(g_rows[:, None] * y_rows.astype(jnp.float32))
        dx_acc = dx_acc.at[tok_ids].add(dx_rows.astype(jnp.float32))
        dg_acc = dg_acc.at[assign].add(dg_rows)
        return (out_acc, dx_acc, dg_acc), (dw_gate, dw_up, dw_down)

    zero_state = (jnp.zeros((TOKENS + 1, D_MODEL), jnp.float32), jnp.zeros((TOKENS + 1, D_MODEL), jnp.float32), jnp.zeros((n_assign + 1,), jnp.float32))
    final_state, weight_grads = lax.scan(one_expert, zero_state, (w_gate, w_up, w_down, filler))
    out_acc, dx_acc, dg_acc = final_state
    dw_gate, dw_up, dw_down = weight_grads
    layer_out = out_acc[:TOKENS].astype(jnp.bfloat16)
    grad_tokens = dx_acc[:TOKENS].astype(jnp.bfloat16)
    grad_gates = dg_acc[:n_assign].reshape(TOKENS, TOP_K)
    return (layer_out, grad_tokens, grad_gates, dw_gate, dw_up, dw_down)
```

```python
import functools

import jax
import jax.numpy as jnp
from jax import lax
from jax.experimental import pallas as pl
from jax.experimental.pallas import tpu as pltpu
from jax.sharding import PartitionSpec as P

F32 = jnp.float32
BF16 = jnp.bfloat16
MESH = pl.DeviceIdType.MESH

TD = 64
D = 2048
F = 1408
K = 6
E = 4
CAP = 24
ND = 8
ROWS = ND * CAP
HALF = D // 2

NT = (((1,), (1,)), ((), ()))
TN = (((0,), (0,)), ((), ()))


def dot(a, b, dims=None):
    if dims is None:
        return jnp.dot(a, b, preferred_element_type=F32)
    return lax.dot_general(a, b, dims, preferred_element_type=F32)


def place():
    y = lax.axis_index('ei')
    o = lax.axis_index('eo')
    x = o // 2
    c = o % 2
    return y, x, c


def flip_if(v, f):
    return v + f - 2 * v * f


def main_kernel(x_hbm, dy_hbm, tbl_hbm, wg_hbm, wu_hbm, wd_hbm,
                y_out, dgt_out, keep_out, send_out, xs_out, us_out, hs_out, dgu_out,
                wgu, wd, xall, dyall, tall, rk, gt, ab, oall, py, rb0, rb1, rb2, rb3, yh,
                dgs, dgr, xsb, usb, hsb, dgb,
                wsem, lsem, snd, rcv, rs_s, rs_r, dg_s, dg_r, osem, psem):
    dp = lax.axis_index('dp')
    y, x, c = place()
    chip = y * 2 + x
    me = chip * 2 + c
    yp, xp = flip_if(y, c), flip_if(x, 1 - c)
    ys, xs = flip_if(y, 1 - c), flip_if(x, c)
    cp, cs, cd = yp * 2 + xp, ys * 2 + xs, (1 - y) * 2 + (1 - x)

    def dev(yy, xx, cc):
        return (dp, yy, xx * 2 + cc)

    partner, prim, sec = dev(y, x, 1 - c), dev(yp, xp, c), dev(ys, xs, c)

    def rcopy(src, dst, ss, rs, target):
        return pltpu.make_async_remote_copy(src_ref=src, dst_ref=dst, send_sem=ss, recv_sem=rs,
                                            device_id=target, device_id_type=MESH)

    def load(src, dst, sem):
        return pltpu.make_async_copy(src, dst, sem)

    def weight_copies(e, sl):
        return (load(wg_hbm.at[e], wgu.at[sl, :, pl.ds(0, F)], wsem.at[sl, 0]),
                load(wu_hbm.at[e], wgu.at[sl, :, pl.ds(F, F)], wsem.at[sl, 1]),
                load(wd_hbm.at[e], wd.at[sl], wsem.at[sl, 2]))

    ins = (load(x_hbm, xall.at[me], lsem.at[0]), load(tbl_hbm, tall.at[me], lsem.at[1]),
           load(dy_hbm, dyall.at[me], lsem.at[2]))
    for cpy in ins:
        cpy.start()
    for e in range(2):
        for cpy in weight_copies(e, e):
            cpy.start()

    barrier = pltpu.get_barrier_semaphore()
    others = [lax.rem(me + k, ND) for k in range(1, ND)]
    for t in others:
        pl.semaphore_signal(barrier, inc=1, device_id=(dp, t // 4, lax.rem(t, 4)), device_id_type=MESH)
    pl.semaphore_wait(barrier, ND - 1)

    bufs = (xall, tall, dyall)
    me_p, me_s, me_d = cp * 2 + c, cs * 2 + c, cd * 2 + c

    def ag_send(st, chunk, k, r, target):
        buf = bufs[st]
        return rcopy(buf.at[chunk], buf.at[chunk], snd.at[st, k], rcv.at[st, r], target)

    def ag_wait(st, chunk, r):
        ag_send(st, chunk, 0, r, partner).wait_recv()

    def ag_open(st):
        ag_send(st, me, 0, 0, prim).start()
        ag_send(st, me, 1, 1, sec).start()
        ag_send(st, me, 2, 3, partner).start()

    def ag_first(st):
        ag_wait(st, me_p, 0)
        ag_send(st, me_p, 3, 2, sec).start()
        ag_send(st, me_p, 4, 5, partner).start()

    def ag_rest(st):
        ag_wait(st, me_s, 1)
        ag_send(st, me_s, 5, 4, partner).start()
        ag_wait(st, me_d, 2)
        ag_send(st, me_d, 6, 6, partner).start()

    def ag_last(st):
        oc = 1 - c
        ag_wait(st, chip * 2 + oc, 3)
        ag_wait(st, cp * 2 + oc, 4)
        ag_wait(st, cs * 2 + oc, 5)
        ag_wait(st, cd * 2 + oc, 6)

    def ag_sent(st):
        for k, (chunk, target) in enumerate(((me, prim), (me, sec), (me, partner), (me_p, sec),
                                             (me_p, partner), (me_s, partner), (me_d, partner))):
            ag_send(st, chunk, k, 0, target).wait_send()

    ins[1].wait()
    ag_open(1)
    ins[0].wait()
    ag_open(0)
    ins[2].wait()
    ag_first(1)
    ag_rest(1)
    ag_first(0)
    ag_open(2)
    ag_last(1)

    li = lax.broadcasted_iota(jnp.int32, (128, 128), 0)
    lj = lax.broadcasted_iota(jnp.int32, (128, 128), 1)
    upper = jnp.where((li // TD == lj // TD) & (li < lj), 1.0, 0.0).astype(BF16)
    for p in range(4):
        tb = tall[2 * p] + tall[2 * p + 1]
        ids, gv = tb[0:8], tb[8:16]
        for e in range(E):
            eid = (me * E + e).astype(F32)
            eq = ids == eid
            hit = jnp.sum(jnp.where(eq, 1.0, 0.0), axis=0, keepdims=True)
            gate = jnp.sum(jnp.where(eq, gv, 0.0), axis=0, keepdims=True)
            hit8 = jnp.broadcast_to(hit, (8, 128))
            rank = dot(hit8.astype(BF16), upper)
            rk[e, :, 128 * p:128 * (p + 1)] = jnp.where(hit8 > 0.5, rank, -1000.0)
            gt[e, :, 128 * p:128 * (p + 1)] = jnp.broadcast_to(gate, (8, 128))

    tok = lax.broadcasted_iota(jnp.int32, (1, ND * TD), 1)
    slot_base = (tok // TD * CAP).astype(F32)
    slot_row = lax.broadcasted_iota(jnp.int32, (ROWS, ND * TD), 0).astype(F32)

    def slot_mask(e):
        return (rk[e][0:1, :] + slot_base) == slot_row

    def put_rows(e, c0, width, val):
        for s in range(ND):
            oall[s, e, :, c0:c0 + width] = val[s * CAP:(s + 1) * CAP]

    ag_rest(0)
    ag_last(0)

    def fwd(e, carry):
        sl = lax.rem(e, 2)
        sel = jnp.where(slot_mask(e), 1.0, 0.0).astype(BF16)

        @pl.when(e > 0)
        def _():
            load(xsb, xs_out.at[e], osem.at[0]).wait()
            load(hsb, hs_out.at[e], osem.at[1]).wait()
        for n in range(4):
            xsb[:, 512 * n:512 * (n + 1)] = dot(sel, xall[:, :, 512 * n:512 * (n + 1)].reshape(ND * TD, 512)).astype(BF16)
        load(xsb, xs_out.at[e], osem.at[0]).start()
        cg, cu, cw = weight_copies(e, sl)
        cg.wait()
        cu.wait()
        for n in range(6):
            lo, w = 256 * n, 256 if n < 5 else 128
            if w == 256:
                a = dot(xsb[...], wgu[sl, :, lo:lo + w])
                b = dot(xsb[...], wgu[sl, :, F + lo:F + lo + w])
            else:
                rhs = jnp.concatenate([wgu[sl, :, lo:lo + w], wgu[sl, :, F + lo:F + lo + w]], axis=1)
                r = dot(xsb[...], rhs)
                a, b = r[:, :w], r[:, w:]
            ab[e, :, lo:lo + w] = a
            ab[e, :, F + lo:F + lo + w] = b
            hsb[:, lo:lo + w] = (a * jax.nn.sigmoid(a) * b).astype(BF16)
        load(hsb, hs_out.at[e], osem.at[1]).start()
        cw.wait()
        for n in range(8):
            put_rows(e, 256 * n, 256, dot(hsb[...], wd[sl, :, 256 * n:256 * (n + 1)]).astype(BF16))

        @pl.when(e < 2)
        def _():
            for cpy in weight_copies(e + 2, sl):
                cpy.start()

        @pl.when(e == 0)
        def _():
            ag_first(2)

        @pl.when(e == 1)
        def _():
            ag_rest(2)
        return carry

    lax.fori_loop(0, E, fwd, 0)
    load(xsb, xs_out.at[E - 1], osem.at[0]).wait()
    load(hsb, hs_out.at[E - 1], osem.at[1]).wait()
    ag_last(2)

    krow = lax.broadcasted_iota(jnp.int32, (2 * E * CAP, 128), 0).astype(F32)
    ptok = lax.broadcasted_iota(jnp.int32, (1, 128), 1)
    pbase = (ptok // TD * (E * CAP)).astype(F32)

    def scatter(gated):
        def body(p, carry):
            sel = jnp.zeros((2 * E * CAP, 128), F32)
            lanes = pl.ds(pl.multiple_of(p * 128, 128), 128)
            for e in range(E):
                m = (rk[e, :, lanes][0:1, :] + pbase + float(e * CAP)) == krow
                m = m & (rk[e, :, lanes][0:1, :] > -1.0)
                sel = jnp.where(m, gt[e, :, lanes][0:1, :] if gated else 1.0, sel)
            if gated:
                g1 = sel.astype(BF16)
                r1 = sel - g1.astype(F32)
                g2 = r1.astype(BF16)
                g3 = (r1 - g2.astype(F32)).astype(BF16)
                lhs = jnp.concatenate([g1, g2, g3], axis=1)
            else:
                lhs = sel.astype(BF16)
            for n in range(4):
                rhs = oall[pl.ds(2 * p, 2), :, :, 512 * n:512 * (n + 1)].reshape(2 * E * CAP, 512)
                r = dot(lhs, rhs, TN)
                if gated:
                    r = r[0:128] + (r[128:256] + r[256:384])
                py[n // 2, p, :, 512 * (n % 2):512 * (n % 2 + 1)] = r
            return carry
        lax.fori_loop(0, 4, body, 0)

    scatter(True)

    rs0 = rcopy(py.at[1 - c], rb0, rs_s.at[0], rs_r.at[0], partner)
    rs1a = rcopy(py.at[c, cd], rb1.at[1], rs_s.at[1], rs_r.at[1], prim)
    rs1b = rcopy(py.at[c, cp], rb1.at[0], rs_s.at[2], rs_r.at[2], prim)
    rs2 = rcopy(py.at[c, cs], rb2, rs_s.at[3], rs_r.at[3], sec)
    rs3 = rcopy(yh.at[1 - c], rb3, rs_s.at[4], rs_r.at[4], partner)
    rs0.start()

    def bwd(n, carry):
        e = E - 1 - n
        sl = lax.rem(e, 2)
        mask = slot_mask(e)
        sel = jnp.where(mask, 1.0, 0.0).astype(BF16)
        gcol = jnp.sum(jnp.where(mask, gt[e][0:1, :], 0.0), axis=1, keepdims=True)

        @pl.when(n > 0)
        def _():
            load(usb, us_out.at[e], osem.at[0]).wait()
            load(dgb, dgu_out.at[e], osem.at[1]).wait()
        dgv = jnp.zeros((ROWS, 1), F32)
        for m in range(4):
            c0 = 512 * m
            dye = dot(sel, dyall[:, :, c0:c0 + 512].reshape(ND * TD, 512))
            usb[:, c0:c0 + 512] = (gcol * dye).astype(BF16)
            oe = jnp.concatenate([oall[s, e, :, c0:c0 + 512] for s in range(ND)], axis=0).astype(F32)
            dgv = dgv + jnp.sum(dye * oe, axis=1, keepdims=True)
        dgrow = jnp.sum(jnp.where(mask, dgv, 0.0), axis=0, keepdims=True)
        dgs[e] = jnp.broadcast_to(dgrow, (8, ND * TD))
        load(usb, us_out.at[e], osem.at[0]).start()
        cg, cu, cw = weight_copies(e, sl)

        @pl.when(n >= 2)
        def _():
            cw.wait()
        for lo, hi in ((0, 768), (768, F)):
            q = dot(wd[sl, lo:hi, :], usb[...], NT).T
            a = ab[e, :, lo:hi]
            b = ab[e, :, F + lo:F + hi]
            s = jax.nn.sigmoid(a)
            dgb[:, F + lo:F + hi] = (q * a * s).astype(BF16)
            dgb[:, lo:hi] = (q * b * s * (1.0 + a * (1.0 - s))).astype(BF16)
        load(dgb, dgu_out.at[e], osem.at[1]).start()

        @pl.when(n >= 2)
        def _():
            cg.wait()
            cu.wait()
        for m in range(4):
            dxt = dot(wgu[sl, 512 * m:512 * (m + 1), :], dgb[...], NT)
            put_rows(e, 512 * m, 512, dxt.T.astype(BF16))

        @pl.when(n < 2)
        def _():
            for cpy in weight_copies(1 - n, sl):
                cpy.start()

        @pl.when(n == 0)
        def _():
            rs0.wait()
            py[c] = py[c] + rb0[...]
            rs1a.start()
            rs1b.start()

        @pl.when(n == 1)
        def _():
            rs1a.wait_recv()
            py[c, cs] = py[c, cs] + rb1[1]
            rs2.start()
        return carry

    lax.fori_loop(0, E, bwd, 0)
    load(usb, us_out.at[0], osem.at[0]).wait()
    load(dgb, dgu_out.at[0], osem.at[1]).wait()

    sends = []
    for i, t in enumerate(others):
        lanes = pl.ds(pl.multiple_of(t // 2 * 128, 128), 128)
        cpy = rcopy(dgs.at[:, :, lanes], dgr.at[me], dg_s.at[i], dg_r.at[me],
                    (dp, t // 4, lax.rem(t, 4)))
        cpy.start()
        sends.append(cpy)
    dgr[me] = dgs[:, :, pl.ds(pl.multiple_of(chip * 128, 128), 128)]

    rs1b.wait_recv()
    rs2.wait_recv()
    own = py[c, chip] + rb1[0] + rb2[...]
    yh[0] = own[0:TD].astype(BF16)
    yh[1] = own[TD:2 * TD].astype(BF16)
    rs3.start()
    rs1a.wait_send()
    rs1b.wait_send()
    rs2.wait_send()
    y_out[:, pl.ds(pl.multiple_of(c * HALF, 128), HALF)] = yh[c]

    scatter(False)
    parts = [load(py.at[c, k], keep_out.at[i], psem.at[i]) for i, k in enumerate((chip, cs, cp, cd))]
    parts += [load(py.at[1 - c, k], send_out.at[i], psem.at[4 + i]) for i, k in enumerate((chip, cp, cs, cd))]
    for cpy in parts:
        cpy.start()

    for i, t in enumerate(others):
        rcopy(dgs.at[:, :, pl.ds(0, 128)], dgr.at[t], dg_s.at[i], dg_r.at[t], partner).wait_recv()
    tb = tall[2 * chip] + tall[2 * chip + 1]
    ids = tb[0:8]
    acc = jnp.zeros((8, 128), F32)
    for t in range(ND):
        for e in range(E):
            acc = acc + jnp.where(ids == float(t * E + e), dgr[t, e], 0.0)
    dgt_out[...] = acc

    rs3.wait_recv()
    y_out[:, pl.ds(pl.multiple_of((1 - c) * HALF, 128), HALF)] = rb3[...]
    rs3.wait_send()
    for st in range(3):
        ag_sent(st)
    for cpy in sends:
        cpy.wait_send()
    for cpy in parts:
        cpy.wait()


def run_main(tok, dy, tbl, wg, wu, wd):
    anys = pl.BlockSpec(memory_space=pl.ANY)
    vm = pl.BlockSpec(memory_space=pltpu.VMEM)
    V = pltpu.VMEM
    S = pltpu.SemaphoreType.DMA
    flops = 2 * E * ROWS * D * F * 6
    return pl.pallas_call(
        main_kernel,
        name='moe_main',
        out_shape=(jax.ShapeDtypeStruct((TD, D), BF16), jax.ShapeDtypeStruct((8, 128), F32),
                   jax.ShapeDtypeStruct((4, 128, HALF), F32), jax.ShapeDtypeStruct((4, 128, HALF), F32),
                   jax.ShapeDtypeStruct((E, ROWS, D), BF16), jax.ShapeDtypeStruct((E, ROWS, D), BF16),
                   jax.ShapeDtypeStruct((E, ROWS, F), BF16), jax.ShapeDtypeStruct((E, ROWS, 2 * F), BF16)),
        in_specs=[anys] * 6,
        out_specs=(vm, vm) + (anys,) * 6,
        scratch_shapes=[
            V((2, D, 2 * F), BF16), V((2, F, D), BF16),
            V((ND, TD, D), BF16), V((ND, TD, D), BF16), V((ND, 16, 128), F32),
            V((E, 8, ND * TD), F32), V((E, 8, ND * TD), F32),
            V((E, ROWS, 2 * F), F32), V((ND, E, CAP, D), BF16),
            V((2, 4, 128, HALF), F32), V((4, 128, HALF), F32), V((2, 128, HALF), F32),
            V((128, HALF), F32), V((TD, HALF), BF16), V((2, TD, HALF), BF16),
            V((E, 8, ND * TD), F32), V((ND, E, 8, 128), F32),
            V((ROWS, D), BF16), V((ROWS, D), BF16), V((ROWS, F), BF16), V((ROWS, 2 * F), BF16),
            S((2, 3)), S((3,)), S((3, 7)), S((3, 7)), S((5,)), S((5,)), S((7,)), S((ND,)), S((2,)), S((8,)),
        ],
        compiler_params=pltpu.CompilerParams(collective_id=0, has_side_effects=True,
                                             vmem_limit_bytes=67043328),
        cost_estimate=pl.CostEstimate(flops=flops, bytes_accessed=120_000_000, transcendentals=0),
    )(tok, dy, tbl, wg, wu, wd)


def down_kernel(h_ref, u_ref, o_ref):
    o_ref[0] = dot(h_ref[0], u_ref[0], TN).astype(BF16)


def run_down(hs, us):
    w = 512
    return pl.pallas_call(
        down_kernel, name='moe_dw_down', grid=(E, D // w),
        in_specs=[pl.BlockSpec((1, ROWS, F), lambda e, n: (e, 0, 0)),
                  pl.BlockSpec((1, ROWS, w), lambda e, n: (e, 0, n))],
        out_specs=pl.BlockSpec((1, F, w), lambda e, n: (e, 0, n)),
        out_shape=jax.ShapeDtypeStruct((E, F, D), BF16),
        compiler_params=pltpu.CompilerParams(vmem_limit_bytes=40 * 2 ** 20),
        cost_estimate=pl.CostEstimate(flops=2 * E * ROWS * D * F, bytes_accessed=28_000_000, transcendentals=0),
    )(hs, us)


def gate_up_kernel(x_ref, g_ref, og_ref, ou_ref):
    r = dot(x_ref[0], g_ref[0], TN)
    og_ref[0] = r[:, :F].astype(BF16)
    ou_ref[0] = r[:, F:].astype(BF16)


def run_gate_up(xs, dgu):
    w = 512
    ospec = pl.BlockSpec((1, w, F), lambda e, n: (e, n, 0))
    return pl.pallas_call(
        gate_up_kernel, name='moe_dw_gate_up', grid=(E, D // w),
        in_specs=[pl.BlockSpec((1, ROWS, w), lambda e, n: (e, 0, n)),
                  pl.BlockSpec((1, ROWS, 2 * F), lambda e, n: (e, 0, 0))],
        out_specs=(ospec, ospec),
        out_shape=(jax.ShapeDtypeStruct((E, D, F), BF16),) * 2,
        compiler_params=pltpu.CompilerParams(vmem_limit_bytes=40 * 2 ** 20),
        cost_estimate=pl.CostEstimate(flops=4 * E * ROWS * D * F, bytes_accessed=55_000_000, transcendentals=0),
    )(xs, dgu)


def exchange_pairs(kind):
    pairs = []
    for y in range(2):
        for x in range(2):
            for c in range(2):
                if kind == 'partner':
                    t = (y, x, 1 - c)
                elif (kind == 'prim') == (c == 0):
                    t = (y, 1 - x, c)
                else:
                    t = (1 - y, x, c)
                pairs.append((y * 4 + x * 2 + c, t[0] * 4 + t[1] * 2 + t[2]))
    return pairs


def solution(mesh):
    tok_spec = P(('dp', 'ei', 'eo'))
    exp_spec = P(('ei', 'eo'))

    def device_step(tok, idx, gate, wg, wu, wd, dy):
        y, x, c = place()
        me = y * 4 + x * 2 + c
        pad = jnp.full((2, TD), -1.0, F32)
        half = jnp.concatenate([idx.T.astype(F32), pad, gate.T, pad], axis=0)
        zero = jnp.zeros_like(half)
        tbl = jnp.where(c == 0, jnp.concatenate([half, zero], axis=1), jnp.concatenate([zero, half], axis=1))

        layer_out, dgt, keep, send, xs, us, hs, dgu = run_main(tok, dy, tbl, wg, wu, wd)

        perm = functools.partial(lax.ppermute, axis_name=('ei', 'eo'))
        r0 = perm(send, perm=exchange_pairs('partner'))
        g_down = run_down(hs, us)
        s1 = keep[2:4] + r0[2:4]
        k1 = keep[0:2] + r0[0:2]
        r1 = perm(s1, perm=exchange_pairs('prim'))
        g_gate, g_up = run_gate_up(xs, dgu)
        t = k1 + r1
        r2 = perm(t[1], perm=exchange_pairs('sec'))
        part = (t[0] + r2).astype(BF16).reshape(2, TD, HALF)
        mine = lax.dynamic_index_in_dim(part, c, 0, keepdims=False)
        theirs = lax.dynamic_index_in_dim(part, 1 - c, 0, keepdims=False)
        r3 = perm(theirs, perm=exchange_pairs('partner'))
        grad_tok = jnp.where(c == 0, jnp.concatenate([mine, r3], axis=1), jnp.concatenate([r3, mine], axis=1))
        dgk = lax.dynamic_slice_in_dim(dgt[:K], c * TD, TD, axis=1).T
        return layer_out, grad_tok, dgk, g_gate, g_up, g_down

    return jax.shard_map(device_step, mesh=mesh,
                         in_specs=(tok_spec, tok_spec, tok_spec, exp_spec, exp_spec, exp_spec, tok_spec),
                         out_specs=(tok_spec, tok_spec, tok_spec, tok_spec, tok_spec, tok_spec), check_vma=False)
```

```python
import functools

import jax
import jax.numpy as jnp
from jax import lax
from jax.experimental import pallas as pl
from jax.experimental.pallas import tpu as pltpu
from jax.sharding import PartitionSpec as P


F32 = jnp.float32
BF16 = jnp.bfloat16
MESH = pl.DeviceIdType.MESH

TD = 64
D = 2048
F = 1408
K = 6
E = 4
CAP = 24
ND = 8
ROWS = ND * CAP

NT = (((1,), (1,)), ((), ()))
TN = (((0,), (0,)), ((), ()))


def dot(a, b, dims=None):
    if dims is None:
        return jnp.dot(a, b, preferred_element_type=F32)
    return lax.dot_general(a, b, dims, preferred_element_type=F32)


def place():
    y = lax.axis_index('ei')
    o = lax.axis_index('eo')
    x = o // 2
    c = o % 2
    return y, x, c


def flip_if(v, f):
    return v + f - 2 * v * f


def main_kernel(x_hbm, dy_hbm, tbl_hbm, wg_hbm, wu_hbm, wd_hbm,
                y_out, dgt_out, s1_out, k1_out, xs_out, us_out, hs_out, dgu_out,
                wgu, wd, xall, dyall, tall, rk, gt, ab, oall, py, rb0, rb1, rb2,
                dgs, dgr, xsb, usb, hsb, dgb,
                wsem, lsem, snd, rcv, rs_s, rs_r, dg_s, dg_r, osem, psem, credit):
    dp = lax.axis_index('dp')
    y, x, c = place()
    chip = y * 2 + x
    me = chip * 2 + c
    yp, xp = flip_if(y, c), flip_if(x, 1 - c)
    ys, xs = flip_if(y, 1 - c), flip_if(x, c)
    cp, cs, cd = yp * 2 + xp, ys * 2 + xs, (1 - y) * 2 + (1 - x)

    def dev(yy, xx, cc):
        return (dp, yy, xx * 2 + cc)

    partner, prim, sec = dev(y, x, 1 - c), dev(yp, xp, c), dev(ys, xs, c)

    def rcopy(src, dst, ss, rs, target):
        return pltpu.make_async_remote_copy(src_ref=src, dst_ref=dst, send_sem=ss, recv_sem=rs,
                                            device_id=target, device_id_type=MESH)

    def load(src, dst, sem):
        return pltpu.make_async_copy(src, dst, sem)

    def weight_copies(e, sl):
        return (load(wg_hbm.at[e], wgu.at[sl, :, pl.ds(0, F)], wsem.at[sl, 0]),
                load(wu_hbm.at[e], wgu.at[sl, :, pl.ds(F, F)], wsem.at[sl, 1]),
                load(wd_hbm.at[e], wd.at[sl], wsem.at[sl, 2]))

    ins = (load(x_hbm, xall.at[me], lsem.at[0]), load(tbl_hbm, tall.at[me], lsem.at[1]),
           load(dy_hbm, dyall.at[me], lsem.at[2]))
    for cpy in ins:
        cpy.start()
    for e in range(2):
        for cpy in weight_copies(e, e):
            cpy.start()

    barrier = pltpu.get_barrier_semaphore()
    others = [lax.rem(me + k, ND) for k in range(1, ND)]
    for t in others:
        pl.semaphore_signal(barrier, inc=1, device_id=(dp, t // 4, lax.rem(t, 4)), device_id_type=MESH)
    pl.semaphore_wait(barrier, ND - 1)

    bufs = (xall, tall, dyall)
    me_p, me_s, me_d = cp * 2 + c, cs * 2 + c, cd * 2 + c

    def ag_send(st, chunk, k, r, target):
        buf = bufs[st]
        return rcopy(buf.at[chunk], buf.at[chunk], snd.at[st, k], rcv.at[st, r], target)

    def ag_wait(st, chunk, r):
        ag_send(st, chunk, 0, r, partner).wait_recv()

    def ag_open(st):
        ag_send(st, me, 0, 0, prim).start()
        ag_send(st, me, 1, 1, sec).start()
        ag_send(st, me, 2, 3, partner).start()

    def ag_first(st):
        ag_wait(st, me_p, 0)
        ag_send(st, me_p, 3, 2, sec).start()
        ag_send(st, me_p, 4, 5, partner).start()

    def ag_rest(st):
        ag_wait(st, me_s, 1)
        ag_send(st, me_s, 5, 4, partner).start()
        ag_wait(st, me_d, 2)
        ag_send(st, me_d, 6, 6, partner).start()

    def ag_last(st):
        oc = 1 - c
        ag_wait(st, chip * 2 + oc, 3)
        ag_wait(st, cp * 2 + oc, 4)
        ag_wait(st, cs * 2 + oc, 5)
        ag_wait(st, cd * 2 + oc, 6)

    def ag_sent(st):
        for k, (chunk, target) in enumerate(((me, prim), (me, sec), (me, partner), (me_p, sec),
                                             (me_p, partner), (me_s, partner), (me_d, partner))):
            ag_send(st, chunk, k, 0, target).wait_send()

    ins[1].wait()
    ag_open(1)
    ins[0].wait()
    ag_open(0)
    ins[2].wait()
    ag_first(1)
    ag_rest(1)
    ag_first(0)
    ag_last(1)

    li = lax.broadcasted_iota(jnp.int32, (128, 128), 0)
    lj = lax.broadcasted_iota(jnp.int32, (128, 128), 1)
    upper = jnp.where((li // TD == lj // TD) & (li < lj), 1.0, 0.0).astype(BF16)
    for p in range(4):
        tb = tall[2 * p] + tall[2 * p + 1]
        ids, gv = tb[0:8], tb[8:16]
        for e in range(E):
            eid = (me * E + e).astype(F32)
            eq = ids == eid
            hit = jnp.sum(jnp.where(eq, 1.0, 0.0), axis=0, keepdims=True)
            gate = jnp.sum(jnp.where(eq, gv, 0.0), axis=0, keepdims=True)
            hit8 = jnp.broadcast_to(hit, (8, 128))
            rank = dot(hit8.astype(BF16), upper)
            rk[e, :, 128 * p:128 * (p + 1)] = jnp.where(hit8 > 0.5, rank, -1000.0)
            gt[e, :, 128 * p:128 * (p + 1)] = jnp.broadcast_to(gate, (8, 128))

    tok = lax.broadcasted_iota(jnp.int32, (1, ND * TD), 1)
    slot_base = (tok // TD * CAP).astype(F32)
    slot_row = lax.broadcasted_iota(jnp.int32, (ROWS, ND * TD), 0).astype(F32)

    def slot_mask(e):
        return (rk[e][0:1, :] + slot_base) == slot_row

    def put_rows(e, c0, width, val):
        for s in range(ND):
            oall[s, e, :, c0:c0 + width] = val[s * CAP:(s + 1) * CAP]

    ag_rest(0)
    ag_open(2)
    ag_last(0)

    def fwd(e, carry):
        sl = lax.rem(e, 2)
        sel = jnp.where(slot_mask(e), 1.0, 0.0).astype(BF16)

        @pl.when(e > 0)
        def _():
            load(xsb, xs_out.at[e], osem.at[0]).wait()
            load(hsb, hs_out.at[e], osem.at[1]).wait()

        for n in range(4):
            xsb[:, 512 * n:512 * (n + 1)] = dot(sel, xall[:, :, 512 * n:512 * (n + 1)].reshape(ND * TD, 512)).astype(BF16)
        load(xsb, xs_out.at[e], osem.at[0]).start()
        cg, cu, cw = weight_copies(e, sl)
        cg.wait()
        cu.wait()
        for n in range(6):
            lo, w = 256 * n, 256 if n < 5 else 128
            if w == 256:
                a = dot(xsb[...], wgu[sl, :, lo:lo + w])
                b = dot(xsb[...], wgu[sl, :, F + lo:F + lo + w])
            else:
                rhs = jnp.concatenate([wgu[sl, :, lo:lo + w], wgu[sl, :, F + lo:F + lo + w]], axis=1)
                r = dot(xsb[...], rhs)
                a, b = r[:, :w], r[:, w:]
            ab[e, :, lo:lo + w] = a
            ab[e, :, F + lo:F + lo + w] = b
            hsb[:, lo:lo + w] = (a * jax.nn.sigmoid(a) * b).astype(BF16)
        load(hsb, hs_out.at[e], osem.at[1]).start()

        @pl.when(e < 2)
        def _():
            for cpy in weight_copies(e + 2, sl)[:2]:
                cpy.start()

        cw.wait()
        for n in range(8):
            put_rows(e, 256 * n, 256, dot(hsb[...], wd[sl, :, 256 * n:256 * (n + 1)]).astype(BF16))

        @pl.when(e < 2)
        def _():
            weight_copies(e + 2, sl)[2].start()

        @pl.when(e == 1)
        def _():
            ag_first(2)

        @pl.when(e == 2)
        def _():
            ag_rest(2)

        return carry

    lax.fori_loop(0, E, fwd, 0)
    load(xsb, xs_out.at[E - 1], osem.at[0]).wait()
    load(hsb, hs_out.at[E - 1], osem.at[1]).wait()
    ag_last(2)

    krow = lax.broadcasted_iota(jnp.int32, (2 * E * CAP, 128), 0).astype(F32)
    ptok = lax.broadcasted_iota(jnp.int32, (1, 128), 1)
    pbase = (ptok // TD * (E * CAP)).astype(F32)

    def scatter(gated, put):
        def body(p, carry):
            sel = jnp.zeros((2 * E * CAP, 128), F32)
            lanes = pl.ds(pl.multiple_of(p * 128, 128), 128)
            for e in range(E):
                m = (rk[e, :, lanes][0:1, :] + pbase + float(e * CAP)) == krow
                sel = jnp.where(m, gt[e, :, lanes][0:1, :] if gated else 1.0, sel)
            if gated:
                g1 = sel.astype(BF16)
                r1 = sel - g1.astype(F32)
                g2 = r1.astype(BF16)
                g3 = (r1 - g2.astype(F32)).astype(BF16)
                lhs = jnp.concatenate([g1, g2, g3], axis=1)
            else:
                lhs = sel.astype(BF16)
            for n in range(4):
                rhs = oall[pl.ds(2 * p, 2), :, :, 512 * n:512 * (n + 1)].reshape(2 * E * CAP, 512)
                r = dot(lhs, rhs, TN)
                if gated:
                    r = r[0:128] + (r[128:256] + r[256:384])
                put(p, slice(512 * n, 512 * (n + 1)), r)
            return carry

        lax.fori_loop(0, 4, body, 0)

    def put_y(p, cols, r):
        py[0, p, :, cols] = r[0:TD]
        py[1, p, :, cols] = r[TD:]

    scatter(True, put_y)

    rs0 = rcopy(py.at[1 - c], rb0, rs_s.at[0], rs_r.at[0], partner)
    rs1a = rcopy(py.at[c, cd], rb1.at[1], rs_s.at[1], rs_r.at[1], prim)
    rs1b = rcopy(py.at[c, cp], rb1.at[0], rs_s.at[2], rs_r.at[2], prim)
    rs2 = rcopy(py.at[c, cs], rb2, rs_s.at[3], rs_r.at[3], sec)
    rs0.start()

    def bwd(n, carry):
        e = E - 1 - n
        sl = lax.rem(e, 2)
        mask = slot_mask(e)
        sel = jnp.where(mask, 1.0, 0.0).astype(BF16)
        gcol = jnp.sum(jnp.where(mask, gt[e][0:1, :], 0.0), axis=1, keepdims=True)

        @pl.when(n > 0)
        def _():
            load(usb, us_out.at[e], osem.at[0]).wait()
            load(dgb, dgu_out.at[e], osem.at[1]).wait()

        dgv = jnp.zeros((ROWS, 1), F32)
        for m in range(4):
            c0 = 512 * m
            dye = dot(sel, dyall[:, :, c0:c0 + 512].reshape(ND * TD, 512))
            usb[:, c0:c0 + 512] = (gcol * dye).astype(BF16)
            oe = jnp.concatenate([oall[s, e, :, c0:c0 + 512] for s in range(ND)], axis=0).astype(F32)
            dgv = dgv + jnp.sum(dye * oe, axis=1, keepdims=True)
        dgrow = jnp.sum(jnp.where(mask, dgv, 0.0), axis=0, keepdims=True)
        dgs[e] = jnp.broadcast_to(dgrow, (8, ND * TD))
        load(usb, us_out.at[e], osem.at[0]).start()
        cg, cu, cw = weight_copies(e, sl)

        @pl.when(n >= 2)
        def _():
            cw.wait()

        for lo, hi in ((0, 768), (768, F)):
            q = dot(wd[sl, lo:hi, :], usb[...], NT).T
            a = ab[e, :, lo:hi]
            b = ab[e, :, F + lo:F + hi]
            s = jax.nn.sigmoid(a)
            dgb[:, F + lo:F + hi] = (q * a * s).astype(BF16)
            dgb[:, lo:hi] = (q * b * s * (1.0 + a * (1.0 - s))).astype(BF16)
        load(dgb, dgu_out.at[e], osem.at[1]).start()

        @pl.when(n < 2)
        def _():
            weight_copies(1 - n, sl)[2].start()

        @pl.when(n == 2)
        def _():
            rs1a.wait_recv()
            py[c, cs] = py[c, cs] + rb1[1]
            rs2.start()

        @pl.when(n >= 2)
        def _():
            cg.wait()
            cu.wait()

        for m in range(4):
            dxt = dot(wgu[sl, 512 * m:512 * (m + 1), :], dgb[...], NT)
            put_rows(e, 512 * m, 512, dxt.T.astype(BF16))

        @pl.when(n < 2)
        def _():
            for cpy in weight_copies(1 - n, sl)[:2]:
                cpy.start()

        @pl.when(n == 0)
        def _():
            rs0.wait()
            py[c] = py[c] + rb0[...]
            rs1a.start()
            rs1b.start()
            pl.semaphore_signal(credit, inc=1, device_id=partner, device_id_type=MESH)

        return carry

    lax.fori_loop(0, E, bwd, 0)
    load(usb, us_out.at[0], osem.at[0]).wait()
    load(dgb, dgu_out.at[0], osem.at[1]).wait()

    sends = []
    for i, t in enumerate(others):
        lanes = pl.ds(pl.multiple_of(t // 2 * 128, 128), 128)
        cpy = rcopy(dgs.at[:, :, lanes], dgr.at[me], dg_s.at[i], dg_r.at[me],
                    (dp, t // 4, lax.rem(t, 4)))
        cpy.start()
        sends.append(cpy)
    dgr[me] = dgs[:, :, pl.ds(pl.multiple_of(chip * 128, 128), 128)]

    def put_dx(p, cols, r):
        ab[p, 0:2 * TD, cols] = r

    scatter(False, put_dx)
    pl.semaphore_wait(credit, 1)
    dx0 = rcopy(ab.at[:, pl.ds(pl.multiple_of((1 - c) * TD, TD), TD), pl.ds(0, D)], rb0,
                rs_s.at[4], rs_r.at[4], partner)
    dx0.start()

    rs1b.wait_recv()
    rs2.wait_recv()
    y_out[...] = (py[c, chip] + rb1[0] + rb2[...]).astype(BF16)

    for i, t in enumerate(others):
        rcopy(dgs.at[:, :, pl.ds(0, 128)], dgr.at[t], dg_s.at[i], dg_r.at[t], partner).wait_recv()
    tb = tall[2 * chip] + tall[2 * chip + 1]
    ids = tb[0:8]
    acc = jnp.zeros((8, 128), F32)
    for t in range(ND):
        for e in range(E):
            acc = acc + jnp.where(ids == float(t * E + e), dgr[t, e], 0.0)
    dgt_out[...] = acc

    dx0.wait_recv()
    own_rows = pl.ds(pl.multiple_of(c * TD, TD), TD)
    parts = []
    for i, (k, out) in enumerate(((cp, s1_out.at[0]), (cd, s1_out.at[1]), (chip, k1_out.at[0]), (cs, k1_out.at[1]))):
        ab[i, 2 * TD:3 * TD, 0:D] = ab[k, own_rows, 0:D] + rb0[k]
        cpy = load(ab.at[i, pl.ds(2 * TD, TD), pl.ds(0, D)], out, psem.at[i])
        cpy.start()
        parts.append(cpy)

    dx0.wait_send()
    rs1a.wait_send()
    rs1b.wait_send()
    rs2.wait_send()
    for st in range(3):
        ag_sent(st)
    for cpy in sends:
        cpy.wait_send()
    for cpy in parts:
        cpy.wait()


def run_main(tok, dy, tbl, wg, wu, wd):
    anys = pl.BlockSpec(memory_space=pl.ANY)
    vm = pl.BlockSpec(memory_space=pltpu.VMEM)
    V = pltpu.VMEM
    S = pltpu.SemaphoreType.DMA
    flops = 2 * E * ROWS * D * F * 6
    return pl.pallas_call(
        main_kernel,
        name='moe_main',
        out_shape=(jax.ShapeDtypeStruct((TD, D), BF16), jax.ShapeDtypeStruct((8, 128), F32),
                   jax.ShapeDtypeStruct((2, TD, D), F32), jax.ShapeDtypeStruct((2, TD, D), F32),
                   jax.ShapeDtypeStruct((E, ROWS, D), BF16), jax.ShapeDtypeStruct((E, ROWS, D), BF16),
                   jax.ShapeDtypeStruct((E, ROWS, F), BF16), jax.ShapeDtypeStruct((E, ROWS, 2 * F), BF16)),
        in_specs=[anys] * 6,
        out_specs=(vm, vm) + (anys,) * 6,
        scratch_shapes=[
            V((2, D, 2 * F), BF16), V((2, F, D), BF16),
            V((ND, TD, D), BF16), V((ND, TD, D), BF16), V((ND, 16, 128), F32),
            V((E, 8, ND * TD), F32), V((E, 8, ND * TD), F32),
            V((E, ROWS, 2 * F), F32), V((ND, E, CAP, D), BF16),
            V((2, 4, TD, D), F32), V((4, TD, D), F32), V((2, TD, D), F32), V((TD, D), F32),
            V((E, 8, ND * TD), F32), V((ND, E, 8, 128), F32),
            V((ROWS, D), BF16), V((ROWS, D), BF16), V((ROWS, F), BF16), V((ROWS, 2 * F), BF16),
            S((2, 3)), S((3,)), S((3, 7)), S((3, 7)), S((5,)), S((5,)), S((7,)), S((ND,)), S((2,)), S((4,)),
            pltpu.SemaphoreType.REGULAR,
        ],
        compiler_params=pltpu.CompilerParams(collective_id=0, has_side_effects=True,
                                             vmem_limit_bytes=67043328),
        cost_estimate=pl.CostEstimate(flops=flops, bytes_accessed=120_000_000, transcendentals=0),
    )(tok, dy, tbl, wg, wu, wd)


RING = 4


def ring_loop(steps, ring, outs, compute):
    def body(i, carry):
        slot = lax.rem(i, ring)

        @pl.when(i >= ring)
        def _():
            for cpy in outs(i - ring, slot):
                cpy.wait()

        compute(i, slot)
        for cpy in outs(i, slot):
            cpy.start()
        return carry

    lax.fori_loop(0, steps, body, 0)
    for k in range(ring):
        i = steps - ring + k
        for cpy in outs(i, i % ring):
            cpy.wait()


def gate_up_kernel(x_hbm, g_hbm, og_hbm, ou_hbm, x_v, g_v, og_v, ou_v, isem, osem):
    def ins(e):
        return (pltpu.make_async_copy(x_hbm.at[e], x_v.at[e], isem.at[e, 0]),
                pltpu.make_async_copy(g_hbm.at[e], g_v.at[e], isem.at[e, 1]))

    for e in range(E):
        for cpy in ins(e):
            cpy.start()

    def outs(i, slot):
        rows = pl.ds(pl.multiple_of(lax.rem(i, 4) * 512, 512), 512)
        return (pltpu.make_async_copy(og_v.at[slot], og_hbm.at[i // 4, rows], osem.at[slot, 0]),
                pltpu.make_async_copy(ou_v.at[slot], ou_hbm.at[i // 4, rows], osem.at[slot, 1]))

    def compute(i, slot):
        e = i // 4

        @pl.when(lax.rem(i, 4) == 0)
        def _():
            for cpy in ins(e):
                cpy.wait()

        cols = pl.ds(pl.multiple_of(lax.rem(i, 4) * 512, 512), 512)
        r = dot(x_v[e, :, cols], g_v[e], TN)
        og_v[slot] = r[:, :F].astype(BF16)
        ou_v[slot] = r[:, F:].astype(BF16)

    ring_loop(4 * E, RING, outs, compute)


def run_gate_up(xs, dgu):
    anys = pl.BlockSpec(memory_space=pl.ANY)
    V = pltpu.VMEM
    return pl.pallas_call(
        gate_up_kernel, name='moe_dw_gate_up',
        in_specs=[anys, anys], out_specs=(anys, anys),
        out_shape=(jax.ShapeDtypeStruct((E, D, F), BF16),) * 2,
        scratch_shapes=[V((E, ROWS, D), BF16), V((E, ROWS, 2 * F), BF16),
                        V((RING, 512, F), BF16), V((RING, 512, F), BF16),
                        pltpu.SemaphoreType.DMA((E, 2)), pltpu.SemaphoreType.DMA((RING, 2))],
        compiler_params=pltpu.CompilerParams(vmem_limit_bytes=67043328),
        cost_estimate=pl.CostEstimate(flops=4 * E * ROWS * D * F, bytes_accessed=55_000_000, transcendentals=0),
    )(xs, dgu)


def down_kernel(h_hbm, u_hbm, o_hbm, h_v, u_v, ht_v, o_v, isem, osem):
    def ins(e):
        return (pltpu.make_async_copy(h_hbm.at[e], h_v.at[e], isem.at[e, 0]),
                pltpu.make_async_copy(u_hbm.at[e], u_v.at[e], isem.at[e, 1]))

    for e in range(E):
        for cpy in ins(e):
            cpy.start()

    def cols(i):
        return pl.ds(pl.multiple_of(lax.rem(i, 4) * 512, 512), 512)

    def outs(i, slot):
        return (pltpu.make_async_copy(o_v.at[slot], o_hbm.at[i // 4, :, cols(i)], osem.at[slot]),)

    def compute(i, slot):
        e = i // 4

        @pl.when(lax.rem(i, 4) == 0)
        def _():
            for cpy in ins(e):
                cpy.wait()
            ht_v[...] = h_v[e].T

        o_v[slot] = dot(ht_v[...], u_v[e, :, cols(i)]).astype(BF16)

    ring_loop(4 * E, RING, outs, compute)


def run_down(hs, us):
    anys = pl.BlockSpec(memory_space=pl.ANY)
    V = pltpu.VMEM
    return pl.pallas_call(
        down_kernel, name='moe_dw_down',
        in_specs=[anys, anys], out_specs=anys,
        out_shape=jax.ShapeDtypeStruct((E, F, D), BF16),
        scratch_shapes=[V((E, ROWS, F), BF16), V((E, ROWS, D), BF16), V((F, ROWS), BF16), V((RING, F, 512), BF16),
                        pltpu.SemaphoreType.DMA((E, 2)), pltpu.SemaphoreType.DMA((RING,))],
        compiler_params=pltpu.CompilerParams(vmem_limit_bytes=67043328),
        cost_estimate=pl.CostEstimate(flops=2 * E * ROWS * D * F, bytes_accessed=28_000_000, transcendentals=0),
    )(hs, us)


def exchange_pairs(kind):
    pairs = []
    for y in range(2):
        for x in range(2):
            for c in range(2):
                if (kind == 'prim') == (c == 0):
                    t = (y, 1 - x, c)
                else:
                    t = (1 - y, x, c)
                pairs.append((y * 4 + x * 2 + c, t[0] * 4 + t[1] * 2 + t[2]))
    return pairs


def solution(mesh):
    tok_spec = P(('dp', 'ei', 'eo'))
    exp_spec = P(('ei', 'eo'))

    def device_step(tok, idx, gate, wg, wu, wd, dy):
        _, _, c = place()
        pad = jnp.full((2, TD), -1.0, F32)
        half = jnp.concatenate([idx.T.astype(F32), pad, gate.T, pad], axis=0)
        zero = jnp.zeros_like(half)
        tbl = jnp.where(c == 0, jnp.concatenate([half, zero], axis=1), jnp.concatenate([zero, half], axis=1))

        layer_out, dgt, s1, k1, xs, us, hs, dgu = run_main(tok, dy, tbl, wg, wu, wd)
        perm = functools.partial(lax.ppermute, axis_name=('ei', 'eo'))
        r1 = perm(s1, perm=exchange_pairs('prim'))
        g_gate, g_up = run_gate_up(xs, dgu)
        g_down = run_down(hs, us)
        t = k1 + r1
        r2 = perm(t[1], perm=exchange_pairs('sec'))
        grad_tok = (t[0] + r2).astype(BF16)
        dgk = lax.dynamic_slice_in_dim(dgt[:K], c * TD, TD, axis=1).T
        return layer_out, grad_tok, dgk, g_gate, g_up, g_down

    return jax.shard_map(device_step, mesh=mesh,
                         in_specs=(tok_spec, tok_spec, tok_spec, exp_spec, exp_spec, exp_spec, tok_spec),
                         out_specs=(tok_spec, tok_spec, tok_spec, tok_spec, tok_spec, tok_spec), check_vma=False)
```

```python
import functools

import jax
import jax.numpy as jnp
from jax import lax
from jax.experimental import pallas as pl
from jax.experimental.pallas import tpu as pltpu
from jax.sharding import PartitionSpec as P


F32 = jnp.float32
BF16 = jnp.bfloat16
MESH = pl.DeviceIdType.MESH

TD = 64
D = 2048
F = 1408
K = 6
E = 4
CAP = 24
ND = 8
ROWS = ND * CAP

NT = (((1,), (1,)), ((), ()))
TN = (((0,), (0,)), ((), ()))


def dot(a, b, dims=None):
    if dims is None:
        return jnp.dot(a, b, preferred_element_type=F32)
    return lax.dot_general(a, b, dims, preferred_element_type=F32)


def place():
    y = lax.axis_index('ei')
    o = lax.axis_index('eo')
    x = o // 2
    c = o % 2
    return y, x, c


def flip_if(v, f):
    return v + f - 2 * v * f


def main_kernel(x_hbm, dy_hbm, id_hbm, ga_hbm, wg_hbm, wu_hbm, wd_hbm,
                y_out, dgt_out, s1_out, own_out, sec_out, xs_out, us_out, hs_out, dgu_out,
                wgu, wd, xall, dyall, idall, gaall, rk, gt, psel, ab, oall, py, rb0, rb1, rb2,
                dgs, dgr, xsb, usb, hsb, dgb,
                wsem, lsem, snd, rcv, rs_s, rs_r, dg_s, dg_r, osem, psem, credit):
    dp = lax.axis_index('dp')
    y, x, c = place()
    chip = y * 2 + x
    me = chip * 2 + c
    yp, xp = flip_if(y, c), flip_if(x, 1 - c)
    ys, xs = flip_if(y, 1 - c), flip_if(x, c)
    cp, cs, cd = yp * 2 + xp, ys * 2 + xs, (1 - y) * 2 + (1 - x)

    def dev(yy, xx, cc):
        return (dp, yy, xx * 2 + cc)

    partner, prim, sec = dev(y, x, 1 - c), dev(yp, xp, c), dev(ys, xs, c)

    def rcopy(src, dst, ss, rs, target):
        return pltpu.make_async_remote_copy(src_ref=src, dst_ref=dst, send_sem=ss, recv_sem=rs,
                                            device_id=target, device_id_type=MESH)

    def load(src, dst, sem):
        return pltpu.make_async_copy(src, dst, sem)

    def weight_copies(e, sl):
        return (load(wg_hbm.at[e], wgu.at[sl, :, pl.ds(0, F)], wsem.at[sl, 0]),
                load(wu_hbm.at[e], wgu.at[sl, :, pl.ds(F, F)], wsem.at[sl, 1]),
                load(wd_hbm.at[e], wd.at[sl], wsem.at[sl, 2]))

    ins = (load(id_hbm, idall.at[me], lsem.at[0]), load(ga_hbm, gaall.at[me], lsem.at[1]),
           load(x_hbm, xall.at[me], lsem.at[2]), load(dy_hbm, dyall.at[me], lsem.at[3]))
    for cpy in ins:
        cpy.start()

    barrier = pltpu.get_barrier_semaphore()
    others = [lax.rem(me + k, ND) for k in range(1, ND)]
    for t in others:
        pl.semaphore_signal(barrier, inc=1, device_id=(dp, t // 4, lax.rem(t, 4)), device_id_type=MESH)
    pl.semaphore_wait(barrier, ND - 1)

    hw = D // 2
    bufs = (lambda k: idall.at[k], lambda k: gaall.at[k],
            lambda k: xall.at[k, :, pl.ds(0, hw)], lambda k: xall.at[k, :, pl.ds(hw, hw)],
            lambda k: dyall.at[k])
    me_p, me_s, me_d = cp * 2 + c, cs * 2 + c, cd * 2 + c

    def ag_send(st, chunk, k, r, target):
        buf = bufs[st]
        return rcopy(buf(chunk), buf(chunk), snd.at[st, k], rcv.at[st, r], target)

    def ag_wait(st, chunk, r):
        ag_send(st, chunk, 0, r, partner).wait_recv()

    def ag_open(st):
        ag_send(st, me, 0, 0, prim).start()
        ag_send(st, me, 1, 1, sec).start()
        ag_send(st, me, 2, 3, partner).start()

    def ag_first(st):
        ag_wait(st, me_p, 0)
        ag_send(st, me_p, 3, 2, sec).start()
        ag_send(st, me_p, 4, 5, partner).start()

    def ag_second(st):
        ag_wait(st, me_s, 1)
        ag_send(st, me_s, 5, 4, partner).start()

    def ag_diag(st):
        ag_wait(st, me_d, 2)
        ag_send(st, me_d, 6, 6, partner).start()

    def ag_last(st):
        oc = 1 - c
        ag_wait(st, chip * 2 + oc, 3)
        ag_wait(st, cp * 2 + oc, 4)
        ag_wait(st, cs * 2 + oc, 5)
        ag_wait(st, cd * 2 + oc, 6)

    def ag_sent(st):
        for k, (chunk, target) in enumerate(((me, prim), (me, sec), (me, partner), (me_p, sec),
                                             (me_p, partner), (me_s, partner), (me_d, partner))):
            ag_send(st, chunk, k, 0, target).wait_send()

    for st in range(2):
        ins[st].wait()
        ag_open(st)
    ins[2].wait()
    ag_open(2)
    ag_open(3)
    ins[3].wait()
    for cpy in weight_copies(0, 0):
        cpy.start()
    for step in (ag_first, ag_second, ag_diag):
        for st in range(2):
            step(st)
    ag_first(2)
    ag_second(2)
    ag_first(3)
    ag_second(3)
    ag_last(0)
    ag_last(1)

    li = lax.broadcasted_iota(jnp.int32, (128, 128), 0)
    lj = lax.broadcasted_iota(jnp.int32, (128, 128), 1)
    upper = jnp.where((li // TD == lj // TD) & (li < lj), 1.0, 0.0).astype(BF16)
    krow = lax.broadcasted_iota(jnp.int32, (2 * E * CAP, 128), 0).astype(F32)
    pbase = (lax.broadcasted_iota(jnp.int32, (1, 128), 1) // TD * (E * CAP)).astype(F32)
    for p in range(4):
        ids = jnp.concatenate([idall[2 * p], idall[2 * p + 1]], axis=1)
        gv = jnp.concatenate([gaall[2 * p], gaall[2 * p + 1]], axis=1)
        sel = jnp.zeros((2 * E * CAP, 128), F32)
        for e in range(E):
            eq = ids == me * E + e
            hit = jnp.sum(jnp.where(eq, 1.0, 0.0), axis=0, keepdims=True)
            gate = jnp.sum(jnp.where(eq, gv, 0.0), axis=0, keepdims=True)
            hit8 = jnp.broadcast_to(hit, (8, 128))
            rank = jnp.where(hit8 > 0.5, dot(hit8.astype(BF16), upper), -1000.0)
            rk[e, :, 128 * p:128 * (p + 1)] = rank
            gt[e, :, 128 * p:128 * (p + 1)] = jnp.broadcast_to(gate, (8, 128))
            sel = jnp.where(rank[0:1, :] + pbase + float(e * CAP) == krow, 1.0, sel)
        psel[p] = sel.astype(BF16)

    tok = lax.broadcasted_iota(jnp.int32, (1, ND * TD), 1)
    slot_base = (tok // TD * CAP).astype(F32)
    slot_row = lax.broadcasted_iota(jnp.int32, (ROWS, ND * TD), 0).astype(F32)

    def slot_mask(e):
        return (rk[e][0:1, :] + slot_base) == slot_row

    def put_rows(e, c0, width, val):
        for s in range(ND):
            oall[s, e, :, c0:c0 + width] = val[s * CAP:(s + 1) * CAP]

    ag_diag(2)
    ag_diag(3)
    for cpy in weight_copies(1, 1):
        cpy.start()
    ag_open(4)
    ag_last(2)
    ag_last(3)

    def fwd(e, carry):
        sl = lax.rem(e, 2)
        sel = jnp.where(slot_mask(e), 1.0, 0.0).astype(BF16)

        @pl.when(e > 0)
        def _():
            load(xsb, xs_out.at[e], osem.at[0]).wait()
            load(hsb, hs_out.at[e], osem.at[1]).wait()

        for n in range(4):
            xsb[:, 512 * n:512 * (n + 1)] = dot(sel, xall[:, :, 512 * n:512 * (n + 1)].reshape(ND * TD, 512)).astype(BF16)
        load(xsb, xs_out.at[e], osem.at[0]).start()
        cg, cu, cw = weight_copies(e, sl)
        cg.wait()
        cu.wait()
        for n in range(6):
            lo, w = 256 * n, 256 if n < 5 else 128
            if w == 256:
                a = dot(xsb[...], wgu[sl, :, lo:lo + w])
                b = dot(xsb[...], wgu[sl, :, F + lo:F + lo + w])
            else:
                rhs = jnp.concatenate([wgu[sl, :, lo:lo + w], wgu[sl, :, F + lo:F + lo + w]], axis=1)
                r = dot(xsb[...], rhs)
                a, b = r[:, :w], r[:, w:]
            ab[e, :, lo:lo + w] = a
            ab[e, :, F + lo:F + lo + w] = b
            hsb[:, lo:lo + w] = (a * jax.nn.sigmoid(a) * b).astype(BF16)
        load(hsb, hs_out.at[e], osem.at[1]).start()

        @pl.when(e < 2)
        def _():
            for cpy in weight_copies(e + 2, sl)[:2]:
                cpy.start()

        cw.wait()
        for n in range(8):
            put_rows(e, 256 * n, 256, dot(hsb[...], wd[sl, :, 256 * n:256 * (n + 1)]).astype(BF16))

        @pl.when(e < 2)
        def _():
            weight_copies(e + 2, sl)[2].start()

        @pl.when(e == 1)
        def _():
            ag_first(4)

        @pl.when(e == 2)
        def _():
            ag_second(4)
            ag_diag(4)

        return carry

    lax.fori_loop(0, E, fwd, 0)
    load(xsb, xs_out.at[E - 1], osem.at[0]).wait()
    load(hsb, hs_out.at[E - 1], osem.at[1]).wait()
    ag_last(4)

    def combine_y(p, carry):
        lanes = pl.ds(pl.multiple_of(p * 128, 128), 128)
        gates = jnp.zeros((2 * E * CAP, 128), F32)
        for e in range(E):
            hit = rk[e, :, lanes][0:1, :] + pbase + float(e * CAP) == krow
            gates = jnp.where(hit, gt[e, :, lanes][0:1, :], gates)
        g1 = gates.astype(BF16)
        rest = gates - g1.astype(F32)
        g2 = rest.astype(BF16)
        g3 = (rest - g2.astype(F32)).astype(BF16)
        lhs = jnp.concatenate([g1, g2, g3], axis=1)
        for n in range(4):
            cols = slice(512 * n, 512 * (n + 1))
            rhs = oall[pl.ds(2 * p, 2), :, :, cols].reshape(2 * E * CAP, 512)
            r = dot(lhs, rhs, TN)
            r = r[0:128] + (r[128:256] + r[256:384])
            py[0, p, :, cols] = r[0:TD]
            py[1, p, :, cols] = r[TD:]
        return carry

    lax.fori_loop(0, 4, combine_y, 0)

    rs0 = rcopy(py.at[1 - c], rb0, rs_s.at[0], rs_r.at[0], partner)
    rs1a = rcopy(py.at[c, cd], rb1.at[1], rs_s.at[1], rs_r.at[1], prim)
    rs1b = rcopy(py.at[c, cp], rb1.at[0], rs_s.at[2], rs_r.at[2], prim)
    rs2 = rcopy(py.at[c, cs], rb2, rs_s.at[3], rs_r.at[3], sec)
    rs0.start()

    def dx_copy(m):
        cols = pl.ds(512 * m, 512)
        return rcopy(ab.at[:, pl.ds(pl.multiple_of((1 - c) * TD, TD), TD), cols], rb0.at[:, :, cols],
                     rs_s.at[4 + m], rs_r.at[4 + m], partner)

    def combine_dx(m):
        cols = slice(512 * m, 512 * (m + 1))

        def body(p, carry):
            rhs = oall[pl.ds(2 * p, 2), :, :, cols].reshape(2 * E * CAP, 512)
            ab[p, 0:2 * TD, cols] = dot(psel[p], rhs, TN)
            return carry

        lax.fori_loop(0, 4, body, 0)
        dx_copy(m).start()

    def bwd(n, carry):
        e = E - 1 - n
        sl = lax.rem(e, 2)
        mask = slot_mask(e)
        sel = jnp.where(mask, 1.0, 0.0).astype(BF16)
        gcol = jnp.sum(jnp.where(mask, gt[e][0:1, :], 0.0), axis=1, keepdims=True)

        @pl.when(n > 0)
        def _():
            load(usb, us_out.at[e], osem.at[0]).wait()
            load(dgb, dgu_out.at[e], osem.at[1]).wait()

        dgv = jnp.zeros((ROWS, 1), F32)
        for m in range(4):
            c0 = 512 * m
            dye = dot(sel, dyall[:, :, c0:c0 + 512].reshape(ND * TD, 512))
            usb[:, c0:c0 + 512] = (gcol * dye).astype(BF16)
            oe = jnp.concatenate([oall[s, e, :, c0:c0 + 512] for s in range(ND)], axis=0).astype(F32)
            dgv = dgv + jnp.sum(dye * oe, axis=1, keepdims=True)
        dgrow = jnp.sum(jnp.where(mask, dgv, 0.0), axis=0, keepdims=True)
        dgs[e] = jnp.broadcast_to(dgrow, (8, ND * TD))
        load(usb, us_out.at[e], osem.at[0]).start()
        cg, cu, cw = weight_copies(e, sl)

        @pl.when(n >= 2)
        def _():
            cw.wait()

        for lo, hi in ((0, 768), (768, F)):
            q = dot(wd[sl, lo:hi, :], usb[...], NT).T
            a = ab[e, :, lo:hi]
            b = ab[e, :, F + lo:F + hi]
            s = jax.nn.sigmoid(a)
            dgb[:, F + lo:F + hi] = (q * a * s).astype(BF16)
            dgb[:, lo:hi] = (q * b * s * (1.0 + a * (1.0 - s))).astype(BF16)
        load(dgb, dgu_out.at[e], osem.at[1]).start()

        @pl.when(n < 2)
        def _():
            weight_copies(1 - n, sl)[2].start()

        @pl.when(n == 2)
        def _():
            rs1a.wait_recv()
            py[c, cs] = py[c, cs] + rb1[1]
            rs2.start()

        @pl.when(n >= 2)
        def _():
            cg.wait()
            cu.wait()

        for m in range(4):
            dxt = dot(wgu[sl, 512 * m:512 * (m + 1), :], dgb[...], NT)
            put_rows(e, 512 * m, 512, dxt.T.astype(BF16))

            @pl.when(n == E - 1)
            def _():
                if m == 0:
                    pl.semaphore_wait(credit, 1)
                combine_dx(m)

        @pl.when(n < 2)
        def _():
            for cpy in weight_copies(1 - n, sl)[:2]:
                cpy.start()

        @pl.when(n == 0)
        def _():
            rs0.wait()
            py[c] = py[c] + rb0[...]
            rs1a.start()
            rs1b.start()
            pl.semaphore_signal(credit, inc=1, device_id=partner, device_id_type=MESH)

        return carry

    lax.fori_loop(0, E, bwd, 0)
    load(usb, us_out.at[0], osem.at[0]).wait()
    load(dgb, dgu_out.at[0], osem.at[1]).wait()

    sends = []
    for i, t in enumerate(others):
        lanes = pl.ds(pl.multiple_of(t // 2 * 128, 128), 128)
        cpy = rcopy(dgs.at[:, :, lanes], dgr.at[me], dg_s.at[i], dg_r.at[me],
                    (dp, t // 4, lax.rem(t, 4)))
        cpy.start()
        sends.append(cpy)
    dgr[me] = dgs[:, :, pl.ds(pl.multiple_of(chip * 128, 128), 128)]

    rs1b.wait_recv()
    rs2.wait_recv()
    y_out[...] = (py[c, chip] + rb1[0] + rb2[...]).astype(BF16)

    own_rows = pl.ds(pl.multiple_of(c * TD, TD), TD)
    dst = ((cp, s1_out.at[0]), (cd, s1_out.at[1]), (chip, own_out), (cs, sec_out))
    parts = []
    for m in range(4):
        dx_copy(m).wait_recv()
        for i, (k, out) in enumerate(dst):
            cols = slice(512 * m, 512 * (m + 1))
            ab[i, 2 * TD:3 * TD, cols] = ab[k, own_rows, cols] + rb0[k, :, cols]
            cpy = load(ab.at[i, pl.ds(2 * TD, TD), pl.ds(512 * m, 512)], out.at[:, pl.ds(512 * m, 512)], psem.at[i, m])
            cpy.start()
            parts.append(cpy)

    for i, t in enumerate(others):
        rcopy(dgs.at[:, :, pl.ds(0, 128)], dgr.at[t], dg_s.at[i], dg_r.at[t], partner).wait_recv()
    ids = idall[me]
    acc = jnp.zeros((K, TD), F32)
    for t in range(ND):
        for e in range(E):
            row = dgr[t, e][0:1, :]
            row = jnp.where(c == 0, row[:, 0:TD], row[:, TD:2 * TD])
            acc = acc + jnp.where(ids == t * E + e, row, 0.0)
    dgt_out[...] = acc

    for m in range(4):
        dx_copy(m).wait_send()
    rs1a.wait_send()
    rs1b.wait_send()
    rs2.wait_send()
    for st in range(5):
        ag_sent(st)
    for cpy in sends:
        cpy.wait_send()
    for cpy in parts:
        cpy.wait()


def run_main(tok, dy, idt, gat, wg, wu, wd):
    anys = pl.BlockSpec(memory_space=pl.ANY)
    vm = pl.BlockSpec(memory_space=pltpu.VMEM)
    V = pltpu.VMEM
    S = pltpu.SemaphoreType.DMA
    flops = 2 * E * ROWS * D * F * 6
    return pl.pallas_call(
        main_kernel,
        name='moe_main',
        out_shape=(jax.ShapeDtypeStruct((TD, D), BF16), jax.ShapeDtypeStruct((K, TD), F32),
                   jax.ShapeDtypeStruct((2, TD, D), F32), jax.ShapeDtypeStruct((TD, D), F32),
                   jax.ShapeDtypeStruct((TD, D), F32),
                   jax.ShapeDtypeStruct((E, ROWS, D), BF16), jax.ShapeDtypeStruct((E, ROWS, D), BF16),
                   jax.ShapeDtypeStruct((E, ROWS, F), BF16), jax.ShapeDtypeStruct((E, ROWS, 2 * F), BF16)),
        in_specs=[anys] * 7,
        out_specs=(vm, vm) + (anys,) * 7,
        scratch_shapes=[
            V((2, D, 2 * F), BF16), V((2, F, D), BF16),
            V((ND, TD, D), BF16), V((ND, TD, D), BF16), V((ND, K, TD), jnp.int32), V((ND, K, TD), F32),
            V((E, 8, ND * TD), F32), V((E, 8, ND * TD), F32), V((4, 2 * E * CAP, 128), BF16),
            V((E, ROWS, 2 * F), F32), V((ND, E, CAP, D), BF16),
            V((2, 4, TD, D), F32), V((4, TD, D), F32), V((2, TD, D), F32), V((TD, D), F32),
            V((E, 8, ND * TD), F32), V((ND, E, 8, 128), F32),
            V((ROWS, D), BF16), V((ROWS, D), BF16), V((ROWS, F), BF16), V((ROWS, 2 * F), BF16),
            S((2, 3)), S((4,)), S((5, 7)), S((5, 7)), S((8,)), S((8,)), S((7,)), S((ND,)), S((2,)), S((4, 4)),
            pltpu.SemaphoreType.REGULAR,
        ],
        compiler_params=pltpu.CompilerParams(collective_id=0, has_side_effects=True,
                                             vmem_limit_bytes=67043328),
        cost_estimate=pl.CostEstimate(flops=flops, bytes_accessed=120_000_000, transcendentals=0),
    )(tok, dy, idt, gat, wg, wu, wd)


RING = 4


def ring_loop(steps, ring, outs, compute):
    def body(i, carry):
        slot = lax.rem(i, ring)

        @pl.when(i >= ring)
        def _():
            for cpy in outs(i - ring, slot):
                cpy.wait()

        compute(i, slot)
        for cpy in outs(i, slot):
            cpy.start()
        return carry

    lax.fori_loop(0, steps, body, 0)
    for k in range(ring):
        i = steps - ring + k
        for cpy in outs(i, i % ring):
            cpy.wait()


def gate_up_kernel(x_hbm, g_hbm, og_hbm, ou_hbm, x_v, g_v, og_v, ou_v, isem, osem):
    def ins(e):
        return (pltpu.make_async_copy(x_hbm.at[e], x_v.at[e], isem.at[e, 0]),
                pltpu.make_async_copy(g_hbm.at[e], g_v.at[e], isem.at[e, 1]))

    for e in range(E):
        for cpy in ins(e):
            cpy.start()

    def outs(i, slot):
        rows = pl.ds(pl.multiple_of(lax.rem(i, 4) * 512, 512), 512)
        return (pltpu.make_async_copy(og_v.at[slot], og_hbm.at[i // 4, rows], osem.at[slot, 0]),
                pltpu.make_async_copy(ou_v.at[slot], ou_hbm.at[i // 4, rows], osem.at[slot, 1]))

    def compute(i, slot):
        e = i // 4

        @pl.when(lax.rem(i, 4) == 0)
        def _():
            for cpy in ins(e):
                cpy.wait()

        cols = pl.ds(pl.multiple_of(lax.rem(i, 4) * 512, 512), 512)
        r = dot(x_v[e, :, cols], g_v[e], TN)
        og_v[slot] = r[:, :F].astype(BF16)
        ou_v[slot] = r[:, F:].astype(BF16)

    ring_loop(4 * E, RING, outs, compute)


def run_gate_up(xs, dgu):
    anys = pl.BlockSpec(memory_space=pl.ANY)
    V = pltpu.VMEM
    return pl.pallas_call(
        gate_up_kernel, name='moe_dw_gate_up',
        in_specs=[anys, anys], out_specs=(anys, anys),
        out_shape=(jax.ShapeDtypeStruct((E, D, F), BF16),) * 2,
        scratch_shapes=[V((E, ROWS, D), BF16), V((E, ROWS, 2 * F), BF16),
                        V((RING, 512, F), BF16), V((RING, 512, F), BF16),
                        pltpu.SemaphoreType.DMA((E, 2)), pltpu.SemaphoreType.DMA((RING, 2))],
        compiler_params=pltpu.CompilerParams(vmem_limit_bytes=67043328),
        cost_estimate=pl.CostEstimate(flops=4 * E * ROWS * D * F, bytes_accessed=55_000_000, transcendentals=0),
    )(xs, dgu)


def down_kernel(h_hbm, u_hbm, o_hbm, h_v, u_v, ht_v, o_v, isem, osem):
    def ins(e):
        return (pltpu.make_async_copy(h_hbm.at[e], h_v.at[e], isem.at[e, 0]),
                pltpu.make_async_copy(u_hbm.at[e], u_v.at[e], isem.at[e, 1]))

    for e in range(E):
        for cpy in ins(e):
            cpy.start()

    def cols(i):
        return pl.ds(pl.multiple_of(lax.rem(i, 4) * 512, 512), 512)

    def outs(i, slot):
        return (pltpu.make_async_copy(o_v.at[slot], o_hbm.at[i // 4, :, cols(i)], osem.at[slot]),)

    def compute(i, slot):
        e = i // 4

        @pl.when(lax.rem(i, 4) == 0)
        def _():
            for cpy in ins(e):
                cpy.wait()
            ht_v[...] = h_v[e].T

        o_v[slot] = dot(ht_v[...], u_v[e, :, cols(i)]).astype(BF16)

    ring_loop(4 * E, RING, outs, compute)


def run_down(hs, us):
    anys = pl.BlockSpec(memory_space=pl.ANY)
    V = pltpu.VMEM
    return pl.pallas_call(
        down_kernel, name='moe_dw_down',
        in_specs=[anys, anys], out_specs=anys,
        out_shape=jax.ShapeDtypeStruct((E, F, D), BF16),
        scratch_shapes=[V((E, ROWS, F), BF16), V((E, ROWS, D), BF16), V((F, ROWS), BF16), V((RING, F, 512), BF16),
                        pltpu.SemaphoreType.DMA((E, 2)), pltpu.SemaphoreType.DMA((RING,))],
        compiler_params=pltpu.CompilerParams(vmem_limit_bytes=67043328),
        cost_estimate=pl.CostEstimate(flops=2 * E * ROWS * D * F, bytes_accessed=28_000_000, transcendentals=0),
    )(hs, us)


def exchange_pairs(kind):
    pairs = []
    for y in range(2):
        for x in range(2):
            for c in range(2):
                if (kind == 'prim') == (c == 0):
                    t = (y, 1 - x, c)
                else:
                    t = (1 - y, x, c)
                pairs.append((y * 4 + x * 2 + c, t[0] * 4 + t[1] * 2 + t[2]))
    return pairs


def solution(mesh):
    tok_spec = P(('dp', 'ei', 'eo'))
    exp_spec = P(('ei', 'eo'))

    def device_step(tok, idx, gate, wg, wu, wd, dy):
        layer_out, dgt, s1, own, second, xs, us, hs, dgu = run_main(tok, dy, idx.T, gate.T, wg, wu, wd)
        perm = functools.partial(lax.ppermute, axis_name=('ei', 'eo'))
        r1 = perm(s1, perm=exchange_pairs('prim'))
        g_gate, g_up = run_gate_up(xs, dgu)
        g_down = run_down(hs, us)
        r2 = perm(second + r1[1], perm=exchange_pairs('sec'))
        grad_tok = (own + r1[0] + r2).astype(BF16)
        dgk = dgt.T
        return layer_out, grad_tok, dgk, g_gate, g_up, g_down

    return jax.shard_map(device_step, mesh=mesh,
                         in_specs=(tok_spec, tok_spec, tok_spec, exp_spec, exp_spec, exp_spec, tok_spec),
                         out_specs=(tok_spec, tok_spec, tok_spec, tok_spec, tok_spec, tok_spec), check_vma=False)
```

```python
import functools

import jax
import jax.numpy as jnp
from jax import lax
from jax.experimental import pallas as pl
from jax.experimental.pallas import tpu as pltpu
from jax.sharding import PartitionSpec as P


F32 = jnp.float32
BF16 = jnp.bfloat16
MESH = pl.DeviceIdType.MESH

TD = 64
D = 2048
F = 1408
K = 6
E = 4
CAP = 24
ND = 8
ROWS = ND * CAP

NT = (((1,), (1,)), ((), ()))
TN = (((0,), (0,)), ((), ()))


def dot(a, b, dims=None):
    if dims is None:
        return jnp.dot(a, b, preferred_element_type=F32)
    return lax.dot_general(a, b, dims, preferred_element_type=F32)


def place():
    y = lax.axis_index('ei')
    o = lax.axis_index('eo')
    x = o // 2
    c = o % 2
    return y, x, c


def flip_if(v, f):
    return v + f - 2 * v * f


def main_kernel(x_hbm, dy_hbm, id_hbm, ga_hbm, wg_hbm, wu_hbm, wd_hbm,
                y_out, dgt_out, s1_out, own_out, sec_out, xs_out, us_out, hs_out, dgu_out,
                wgu, wd, xall, dyall, idall, gaall, rk, gt, psel, ab, oall, py, rb0, rb1, rb2,
                dgs, dgr, xsb, usb, hsb, dgb,
                wsem, lsem, snd, rcv, rs_s, rs_r, dg_s, dg_r, osem, psem, credit):
    dp = lax.axis_index('dp')
    y, x, c = place()
    chip = y * 2 + x
    me = chip * 2 + c
    yp, xp = flip_if(y, c), flip_if(x, 1 - c)
    ys, xs = flip_if(y, 1 - c), flip_if(x, c)
    cp, cs, cd = yp * 2 + xp, ys * 2 + xs, (1 - y) * 2 + (1 - x)

    def dev(yy, xx, cc):
        return (dp, yy, xx * 2 + cc)

    partner, prim, sec = dev(y, x, 1 - c), dev(yp, xp, c), dev(ys, xs, c)

    def rcopy(src, dst, ss, rs, target):
        return pltpu.make_async_remote_copy(src_ref=src, dst_ref=dst, send_sem=ss, recv_sem=rs,
                                            device_id=target, device_id_type=MESH)

    def load(src, dst, sem):
        return pltpu.make_async_copy(src, dst, sem)

    def start_gate_up(e, sl):
        for lo in range(0, D, 256):
            rows = pl.ds(lo, 256)
            load(wg_hbm.at[e, rows], wgu.at[sl, rows, pl.ds(0, F)], wsem.at[sl, 0]).start()
            load(wu_hbm.at[e, rows], wgu.at[sl, rows, pl.ds(F, F)], wsem.at[sl, 1]).start()

    def start_down(e, sl):
        for lo in range(0, F, 176):
            rows = pl.ds(lo, 176)
            load(wd_hbm.at[e, rows], wd.at[sl, rows], wsem.at[sl, 2]).start()

    def wait_gate_up(e, sl):
        load(wg_hbm.at[e], wgu.at[sl, :, pl.ds(0, F)], wsem.at[sl, 0]).wait()
        load(wu_hbm.at[e], wgu.at[sl, :, pl.ds(F, F)], wsem.at[sl, 1]).wait()

    def wait_down(e, sl):
        load(wd_hbm.at[e], wd.at[sl], wsem.at[sl, 2]).wait()

    ins = (load(id_hbm, idall.at[me], lsem.at[0]), load(ga_hbm, gaall.at[me], lsem.at[1]),
           load(x_hbm, xall.at[me], lsem.at[2]), load(dy_hbm, dyall.at[me], lsem.at[3]))
    for cpy in ins:
        cpy.start()

    barrier = pltpu.get_barrier_semaphore()
    others = [lax.rem(me + k, ND) for k in range(1, ND)]
    for t in others:
        pl.semaphore_signal(barrier, inc=1, device_id=(dp, t // 4, lax.rem(t, 4)), device_id_type=MESH)
    pl.semaphore_wait(barrier, ND - 1)

    hw = D // 2
    bufs = (lambda k: idall.at[k], lambda k: gaall.at[k],
            lambda k: xall.at[k, :, pl.ds(0, hw)], lambda k: xall.at[k, :, pl.ds(hw, hw)],
            lambda k: dyall.at[k])
    me_p, me_s, me_d = cp * 2 + c, cs * 2 + c, cd * 2 + c

    def ag_send(st, chunk, k, r, target):
        buf = bufs[st]
        return rcopy(buf(chunk), buf(chunk), snd.at[st, k], rcv.at[st, r], target)

    def ag_wait(st, chunk, r):
        ag_send(st, chunk, 0, r, partner).wait_recv()

    def ag_open(st):
        ag_send(st, me, 0, 0, prim).start()
        ag_send(st, me, 1, 1, sec).start()
        ag_send(st, me, 2, 3, partner).start()

    def ag_first(st):
        ag_wait(st, me_p, 0)
        ag_send(st, me_p, 3, 2, sec).start()
        ag_send(st, me_p, 4, 5, partner).start()

    def ag_second(st):
        ag_wait(st, me_s, 1)
        ag_send(st, me_s, 5, 4, partner).start()

    def ag_diag(st):
        ag_wait(st, me_d, 2)
        ag_send(st, me_d, 6, 6, partner).start()

    def ag_last(st):
        oc = 1 - c
        ag_wait(st, chip * 2 + oc, 3)
        ag_wait(st, cp * 2 + oc, 4)
        ag_wait(st, cs * 2 + oc, 5)
        ag_wait(st, cd * 2 + oc, 6)

    def ag_sent(st):
        for k, (chunk, target) in enumerate(((me, prim), (me, sec), (me, partner), (me_p, sec),
                                             (me_p, partner), (me_s, partner), (me_d, partner))):
            ag_send(st, chunk, k, 0, target).wait_send()

    for st in range(2):
        ins[st].wait()
        ag_open(st)
    ins[2].wait()
    ag_open(2)
    ag_open(3)
    ins[3].wait()
    start_gate_up(0, 0)
    start_down(0, 0)
    for step in (ag_first, ag_second, ag_diag):
        for st in range(2):
            step(st)
    ag_first(2)
    ag_second(2)
    ag_first(3)
    ag_second(3)
    ag_last(0)
    ag_last(1)

    li = lax.broadcasted_iota(jnp.int32, (128, 128), 0)
    lj = lax.broadcasted_iota(jnp.int32, (128, 128), 1)
    upper = jnp.where((li // TD == lj // TD) & (li < lj), 1.0, 0.0).astype(BF16)
    krow = lax.broadcasted_iota(jnp.int32, (2 * E * CAP, 128), 0).astype(F32)
    pbase = (lax.broadcasted_iota(jnp.int32, (1, 128), 1) // TD * (E * CAP)).astype(F32)
    for p in range(4):
        ids = jnp.concatenate([idall[2 * p], idall[2 * p + 1]], axis=1)
        gv = jnp.concatenate([gaall[2 * p], gaall[2 * p + 1]], axis=1)
        sel = jnp.zeros((2 * E * CAP, 128), F32)
        for e in range(E):
            eq = ids == me * E + e
            hit = jnp.sum(jnp.where(eq, 1.0, 0.0), axis=0, keepdims=True)
            gate = jnp.sum(jnp.where(eq, gv, 0.0), axis=0, keepdims=True)
            hit8 = jnp.broadcast_to(hit, (8, 128))
            rank = jnp.where(hit8 > 0.5, dot(hit8.astype(BF16), upper), -1000.0)
            rk[e, :, 128 * p:128 * (p + 1)] = rank
            gt[e, :, 128 * p:128 * (p + 1)] = jnp.broadcast_to(gate, (8, 128))
            sel = jnp.where(rank[0:1, :] + pbase + float(e * CAP) == krow, 1.0, sel)
        psel[p] = sel.astype(BF16)

    tok = lax.broadcasted_iota(jnp.int32, (1, ND * TD), 1)
    slot_base = (tok // TD * CAP).astype(F32)
    slot_row = lax.broadcasted_iota(jnp.int32, (ROWS, ND * TD), 0).astype(F32)

    def slot_mask(e):
        return (rk[e][0:1, :] + slot_base) == slot_row

    def put_rows(e, c0, width, val):
        for s in range(ND):
            oall[s, e, :, c0:c0 + width] = val[s * CAP:(s + 1) * CAP]

    ag_diag(2)
    ag_diag(3)
    start_gate_up(1, 1)
    start_down(1, 1)
    ag_open(4)
    ag_last(2)
    ag_last(3)

    def fwd(e, carry):
        sl = lax.rem(e, 2)
        sel = jnp.where(slot_mask(e), 1.0, 0.0).astype(BF16)

        @pl.when(e > 0)
        def _():
            load(xsb, xs_out.at[e], osem.at[0]).wait()
            load(hsb, hs_out.at[e], osem.at[1]).wait()

        for n in range(4):
            xsb[:, 512 * n:512 * (n + 1)] = dot(sel, xall[:, :, 512 * n:512 * (n + 1)].reshape(ND * TD, 512)).astype(BF16)
        load(xsb, xs_out.at[e], osem.at[0]).start()
        wait_gate_up(e, sl)
        for n in range(6):
            lo, w = 256 * n, 256 if n < 5 else 128
            if w == 256:
                a = dot(xsb[...], wgu[sl, :, lo:lo + w])
                b = dot(xsb[...], wgu[sl, :, F + lo:F + lo + w])
            else:
                rhs = jnp.concatenate([wgu[sl, :, lo:lo + w], wgu[sl, :, F + lo:F + lo + w]], axis=1)
                r = dot(xsb[...], rhs)
                a, b = r[:, :w], r[:, w:]
            ab[e, :, lo:lo + w] = a
            ab[e, :, F + lo:F + lo + w] = b
            hsb[:, lo:lo + w] = (a * jax.nn.sigmoid(a) * b).astype(BF16)
        load(hsb, hs_out.at[e], osem.at[1]).start()

        @pl.when(e < 2)
        def _():
            start_gate_up(e + 2, sl)

        wait_down(e, sl)
        for n in range(8):
            put_rows(e, 256 * n, 256, dot(hsb[...], wd[sl, :, 256 * n:256 * (n + 1)]).astype(BF16))

        @pl.when(e < 2)
        def _():
            start_down(e + 2, sl)

        @pl.when(e == 1)
        def _():
            ag_first(4)

        @pl.when(e == 2)
        def _():
            ag_second(4)
            ag_diag(4)

        return carry

    lax.fori_loop(0, E, fwd, 0)
    load(xsb, xs_out.at[E - 1], osem.at[0]).wait()
    load(hsb, hs_out.at[E - 1], osem.at[1]).wait()
    ag_last(4)

    def combine_y(p, carry):
        lanes = pl.ds(pl.multiple_of(p * 128, 128), 128)
        gates = jnp.zeros((2 * E * CAP, 128), F32)
        for e in range(E):
            hit = rk[e, :, lanes][0:1, :] + pbase + float(e * CAP) == krow
            gates = jnp.where(hit, gt[e, :, lanes][0:1, :], gates)
        g1 = gates.astype(BF16)
        rest = gates - g1.astype(F32)
        g2 = rest.astype(BF16)
        g3 = (rest - g2.astype(F32)).astype(BF16)
        lhs = jnp.concatenate([g1, g2, g3], axis=1)
        for n in range(4):
            cols = slice(512 * n, 512 * (n + 1))
            rhs = oall[pl.ds(2 * p, 2), :, :, cols].reshape(2 * E * CAP, 512)
            r = dot(lhs, rhs, TN)
            r = r[0:128] + (r[128:256] + r[256:384])
            py[0, p, :, cols] = r[0:TD]
            py[1, p, :, cols] = r[TD:]
        return carry

    lax.fori_loop(0, 4, combine_y, 0)

    rs0 = rcopy(py.at[1 - c], rb0, rs_s.at[0], rs_r.at[0], partner)
    rs1a = rcopy(py.at[c, cd], rb1.at[1], rs_s.at[1], rs_r.at[1], prim)
    rs1b = rcopy(py.at[c, cp], rb1.at[0], rs_s.at[2], rs_r.at[2], prim)
    rs2 = rcopy(py.at[c, cs], rb2, rs_s.at[3], rs_r.at[3], sec)
    rs0.start()

    def dx_copy(m):
        cols = pl.ds(512 * m, 512)
        return rcopy(ab.at[:, pl.ds(pl.multiple_of((1 - c) * TD, TD), TD), cols], rb0.at[:, :, cols],
                     rs_s.at[4 + m], rs_r.at[4 + m], partner)

    def combine_dx(m):
        cols = slice(512 * m, 512 * (m + 1))

        def body(p, carry):
            rhs = oall[pl.ds(2 * p, 2), :, :, cols].reshape(2 * E * CAP, 512)
            ab[p, 0:2 * TD, cols] = dot(psel[p], rhs, TN)
            return carry

        lax.fori_loop(0, 4, body, 0)
        dx_copy(m).start()

    def bwd(n, carry):
        e = E - 1 - n
        sl = lax.rem(e, 2)
        mask = slot_mask(e)
        sel = jnp.where(mask, 1.0, 0.0).astype(BF16)
        gcol = jnp.sum(jnp.where(mask, gt[e][0:1, :], 0.0), axis=1, keepdims=True)

        @pl.when(n > 0)
        def _():
            load(usb, us_out.at[e], osem.at[0]).wait()
            load(dgb, dgu_out.at[e], osem.at[1]).wait()

        dgv = jnp.zeros((ROWS, 1), F32)
        for m in range(4):
            c0 = 512 * m
            dye = dot(sel, dyall[:, :, c0:c0 + 512].reshape(ND * TD, 512))
            usb[:, c0:c0 + 512] = (gcol * dye).astype(BF16)
            oe = jnp.concatenate([oall[s, e, :, c0:c0 + 512] for s in range(ND)], axis=0).astype(F32)
            dgv = dgv + jnp.sum(dye * oe, axis=1, keepdims=True)
        dgrow = jnp.sum(jnp.where(mask, dgv, 0.0), axis=0, keepdims=True)
        dgs[e] = jnp.broadcast_to(dgrow, (8, ND * TD))
        load(usb, us_out.at[e], osem.at[0]).start()

        @pl.when(n >= 2)
        def _():
            wait_down(e, sl)

        for lo, hi in ((0, 768), (768, F)):
            q = dot(wd[sl, lo:hi, :], usb[...], NT).T
            a = ab[e, :, lo:hi]
            b = ab[e, :, F + lo:F + hi]
            s = jax.nn.sigmoid(a)
            dgb[:, F + lo:F + hi] = (q * a * s).astype(BF16)
            dgb[:, lo:hi] = (q * b * s * (1.0 + a * (1.0 - s))).astype(BF16)
        load(dgb, dgu_out.at[e], osem.at[1]).start()

        @pl.when(n < 2)
        def _():
            start_down(1 - n, sl)

        @pl.when(n == 2)
        def _():
            rs1a.wait_recv()
            py[c, cs] = py[c, cs] + rb1[1]
            rs2.start()

        @pl.when(n >= 2)
        def _():
            wait_gate_up(e, sl)

        for m in range(4):
            dxt = dot(wgu[sl, 512 * m:512 * (m + 1), :], dgb[...], NT)
            put_rows(e, 512 * m, 512, dxt.T.astype(BF16))

            @pl.when(n == E - 1)
            def _():
                if m == 0:
                    pl.semaphore_wait(credit, 1)
                combine_dx(m)

        @pl.when(n < 2)
        def _():
            start_gate_up(1 - n, sl)

        @pl.when(n == 0)
        def _():
            rs0.wait()
            py[c] = py[c] + rb0[...]
            rs1a.start()
            rs1b.start()
            pl.semaphore_signal(credit, inc=1, device_id=partner, device_id_type=MESH)

        return carry

    lax.fori_loop(0, E, bwd, 0)
    load(usb, us_out.at[0], osem.at[0]).wait()
    load(dgb, dgu_out.at[0], osem.at[1]).wait()

    sends = []
    for i, t in enumerate(others):
        lanes = pl.ds(pl.multiple_of(t // 2 * 128, 128), 128)
        cpy = rcopy(dgs.at[:, :, lanes], dgr.at[me], dg_s.at[i], dg_r.at[me],
                    (dp, t // 4, lax.rem(t, 4)))
        cpy.start()
        sends.append(cpy)
    dgr[me] = dgs[:, :, pl.ds(pl.multiple_of(chip * 128, 128), 128)]

    rs1b.wait_recv()
    rs2.wait_recv()
    y_out[...] = (py[c, chip] + rb1[0] + rb2[...]).astype(BF16)

    own_rows = pl.ds(pl.multiple_of(c * TD, TD), TD)
    dst = ((cp, s1_out.at[0]), (cd, s1_out.at[1]), (chip, own_out), (cs, sec_out))
    parts = []
    for m in range(4):
        dx_copy(m).wait_recv()
        for i, (k, out) in enumerate(dst):
            cols = slice(512 * m, 512 * (m + 1))
            ab[i, 2 * TD:3 * TD, cols] = ab[k, own_rows, cols] + rb0[k, :, cols]
            cpy = load(ab.at[i, pl.ds(2 * TD, TD), pl.ds(512 * m, 512)], out.at[:, pl.ds(512 * m, 512)], psem.at[i, m])
            cpy.start()
            parts.append(cpy)

    for i, t in enumerate(others):
        rcopy(dgs.at[:, :, pl.ds(0, 128)], dgr.at[t], dg_s.at[i], dg_r.at[t], partner).wait_recv()
    ids = idall[me]
    acc = jnp.zeros((K, TD), F32)
    for t in range(ND):
        for e in range(E):
            row = dgr[t, e][0:1, :]
            row = jnp.where(c == 0, row[:, 0:TD], row[:, TD:2 * TD])
            acc = acc + jnp.where(ids == t * E + e, row, 0.0)
    dgt_out[...] = acc

    for m in range(4):
        dx_copy(m).wait_send()
    rs1a.wait_send()
    rs1b.wait_send()
    rs2.wait_send()
    for st in range(5):
        ag_sent(st)
    for cpy in sends:
        cpy.wait_send()
    for cpy in parts:
        cpy.wait()


def run_main(tok, dy, idt, gat, wg, wu, wd):
    anys = pl.BlockSpec(memory_space=pl.ANY)
    vm = pl.BlockSpec(memory_space=pltpu.VMEM)
    V = pltpu.VMEM
    S = pltpu.SemaphoreType.DMA
    flops = 2 * E * ROWS * D * F * 6
    return pl.pallas_call(
        main_kernel,
        name='moe_main',
        out_shape=(jax.ShapeDtypeStruct((TD, D), BF16), jax.ShapeDtypeStruct((K, TD), F32),
                   jax.ShapeDtypeStruct((2, TD, D), F32), jax.ShapeDtypeStruct((TD, D), F32),
                   jax.ShapeDtypeStruct((TD, D), F32),
                   jax.ShapeDtypeStruct((E, ROWS, D), BF16), jax.ShapeDtypeStruct((E, ROWS, D), BF16),
                   jax.ShapeDtypeStruct((E, ROWS, F), BF16), jax.ShapeDtypeStruct((E, ROWS, 2 * F), BF16)),
        in_specs=[anys] * 7,
        out_specs=(vm, vm) + (anys,) * 7,
        scratch_shapes=[
            V((2, D, 2 * F), BF16), V((2, F, D), BF16),
            V((ND, TD, D), BF16), V((ND, TD, D), BF16), V((ND, K, TD), jnp.int32), V((ND, K, TD), F32),
            V((E, 8, ND * TD), F32), V((E, 8, ND * TD), F32), V((4, 2 * E * CAP, 128), BF16),
            V((E, ROWS, 2 * F), F32), V((ND, E, CAP, D), BF16),
            V((2, 4, TD, D), F32), V((4, TD, D), F32), V((2, TD, D), F32), V((TD, D), F32),
            V((E, 8, ND * TD), F32), V((ND, E, 8, 128), F32),
            V((ROWS, D), BF16), V((ROWS, D), BF16), V((ROWS, F), BF16), V((ROWS, 2 * F), BF16),
            S((2, 3)), S((4,)), S((5, 7)), S((5, 7)), S((8,)), S((8,)), S((7,)), S((ND,)), S((2,)), S((4, 4)),
            pltpu.SemaphoreType.REGULAR,
        ],
        compiler_params=pltpu.CompilerParams(collective_id=0, has_side_effects=True,
                                             vmem_limit_bytes=67043328),
        cost_estimate=pl.CostEstimate(flops=flops, bytes_accessed=120_000_000, transcendentals=0),
    )(tok, dy, idt, gat, wg, wu, wd)


RING = 4


def ring_loop(steps, ring, outs, compute):
    def body(i, carry):
        slot = lax.rem(i, ring)

        @pl.when(i >= ring)
        def _():
            for cpy in outs(i - ring, slot):
                cpy.wait()

        compute(i, slot)
        for cpy in outs(i, slot):
            cpy.start()
        return carry

    lax.fori_loop(0, steps, body, 0)
    for k in range(ring):
        i = steps - ring + k
        for cpy in outs(i, i % ring):
            cpy.wait()


def gate_up_kernel(x_hbm, g_hbm, og_hbm, ou_hbm, x_v, g_v, og_v, ou_v, isem, osem):
    def ins(e):
        return (pltpu.make_async_copy(x_hbm.at[e], x_v.at[e], isem.at[e, 0]),
                pltpu.make_async_copy(g_hbm.at[e], g_v.at[e], isem.at[e, 1]))

    for e in range(E):
        for cpy in ins(e):
            cpy.start()

    def outs(i, slot):
        rows = pl.ds(pl.multiple_of(lax.rem(i, 4) * 512, 512), 512)
        return (pltpu.make_async_copy(og_v.at[slot], og_hbm.at[i // 4, rows], osem.at[slot, 0]),
                pltpu.make_async_copy(ou_v.at[slot], ou_hbm.at[i // 4, rows], osem.at[slot, 1]))

    def compute(i, slot):
        e = i // 4

        @pl.when(lax.rem(i, 4) == 0)
        def _():
            for cpy in ins(e):
                cpy.wait()

        cols = pl.ds(pl.multiple_of(lax.rem(i, 4) * 512, 512), 512)
        r = dot(x_v[e, :, cols], g_v[e], TN)
        og_v[slot] = r[:, :F].astype(BF16)
        ou_v[slot] = r[:, F:].astype(BF16)

    ring_loop(4 * E, RING, outs, compute)


def run_gate_up(xs, dgu):
    anys = pl.BlockSpec(memory_space=pl.ANY)
    V = pltpu.VMEM
    return pl.pallas_call(
        gate_up_kernel, name='moe_dw_gate_up',
        in_specs=[anys, anys], out_specs=(anys, anys),
        out_shape=(jax.ShapeDtypeStruct((E, D, F), BF16),) * 2,
        scratch_shapes=[V((E, ROWS, D), BF16), V((E, ROWS, 2 * F), BF16),
                        V((RING, 512, F), BF16), V((RING, 512, F), BF16),
                        pltpu.SemaphoreType.DMA((E, 2)), pltpu.SemaphoreType.DMA((RING, 2))],
        compiler_params=pltpu.CompilerParams(vmem_limit_bytes=67043328),
        cost_estimate=pl.CostEstimate(flops=4 * E * ROWS * D * F, bytes_accessed=55_000_000, transcendentals=0),
    )(xs, dgu)


def down_kernel(h_hbm, u_hbm, o_hbm, h_v, u_v, ht_v, o_v, isem, osem):
    def ins(e):
        return (pltpu.make_async_copy(h_hbm.at[e], h_v.at[e], isem.at[e, 0]),
                pltpu.make_async_copy(u_hbm.at[e], u_v.at[e], isem.at[e, 1]))

    for e in range(E):
        for cpy in ins(e):
            cpy.start()

    def cols(i):
        return pl.ds(pl.multiple_of(lax.rem(i, 4) * 512, 512), 512)

    def outs(i, slot):
        return (pltpu.make_async_copy(o_v.at[slot], o_hbm.at[i // 4, :, cols(i)], osem.at[slot]),)

    def compute(i, slot):
        e = i // 4

        @pl.when(lax.rem(i, 4) == 0)
        def _():
            for cpy in ins(e):
                cpy.wait()
            ht_v[...] = h_v[e].T

        o_v[slot] = dot(ht_v[...], u_v[e, :, cols(i)]).astype(BF16)

    ring_loop(4 * E, RING, outs, compute)


def run_down(hs, us):
    anys = pl.BlockSpec(memory_space=pl.ANY)
    V = pltpu.VMEM
    return pl.pallas_call(
        down_kernel, name='moe_dw_down',
        in_specs=[anys, anys], out_specs=anys,
        out_shape=jax.ShapeDtypeStruct((E, F, D), BF16),
        scratch_shapes=[V((E, ROWS, F), BF16), V((E, ROWS, D), BF16), V((F, ROWS), BF16), V((RING, F, 512), BF16),
                        pltpu.SemaphoreType.DMA((E, 2)), pltpu.SemaphoreType.DMA((RING,))],
        compiler_params=pltpu.CompilerParams(vmem_limit_bytes=67043328),
        cost_estimate=pl.CostEstimate(flops=2 * E * ROWS * D * F, bytes_accessed=28_000_000, transcendentals=0),
    )(hs, us)


def exchange_pairs(kind):
    pairs = []
    for y in range(2):
        for x in range(2):
            for c in range(2):
                if (kind == 'prim') == (c == 0):
                    t = (y, 1 - x, c)
                else:
                    t = (1 - y, x, c)
                pairs.append((y * 4 + x * 2 + c, t[0] * 4 + t[1] * 2 + t[2]))
    return pairs


def solution(mesh):
    tok_spec = P(('dp', 'ei', 'eo'))
    exp_spec = P(('ei', 'eo'))

    def device_step(tok, idx, gate, wg, wu, wd, dy):
        layer_out, dgt, s1, own, second, xs, us, hs, dgu = run_main(tok, dy, idx.T, gate.T, wg, wu, wd)
        perm = functools.partial(lax.ppermute, axis_name=('ei', 'eo'))
        r1 = perm(s1, perm=exchange_pairs('prim'))
        g_gate, g_up = run_gate_up(xs, dgu)
        g_down = run_down(hs, us)
        r2 = perm(second + r1[1], perm=exchange_pairs('sec'))
        grad_tok = (own + r1[0] + r2).astype(BF16)
        dgk = dgt.T
        return layer_out, grad_tok, dgk, g_gate, g_up, g_down

    return jax.shard_map(device_step, mesh=mesh,
                         in_specs=(tok_spec, tok_spec, tok_spec, exp_spec, exp_spec, exp_spec, tok_spec),
                         out_specs=(tok_spec, tok_spec, tok_spec, tok_spec, tok_spec, tok_spec), check_vma=False)
```

```python
import functools

import jax
import jax.numpy as jnp
from jax import lax
from jax.experimental import pallas as pl
from jax.experimental.pallas import tpu as pltpu
from jax.sharding import PartitionSpec as P


F32 = jnp.float32
BF16 = jnp.bfloat16
MESH = pl.DeviceIdType.MESH

TD = 64
D = 2048
F = 1408
K = 6
E = 4
CAP = 24
ND = 8
ROWS = ND * CAP

NT = (((1,), (1,)), ((), ()))
TN = (((0,), (0,)), ((), ()))


def dot(a, b, dims=None):
    if dims is None:
        return jnp.dot(a, b, preferred_element_type=F32)
    return lax.dot_general(a, b, dims, preferred_element_type=F32)


def place():
    y = lax.axis_index('ei')
    o = lax.axis_index('eo')
    x = o // 2
    c = o % 2
    return y, x, c


def flip_if(v, f):
    return v + f - 2 * v * f


def main_kernel(x_hbm, dy_hbm, id_hbm, ga_hbm, wg_hbm, wu_hbm, wd_hbm,
                y_out, dgt_out, s1_out, own_out, sec_out, xs_out, us_out, hs_out, dgu_out,
                wgu, wd, xall, dyall, idall, gaall, rk, gt, psel, ab, oall, py, rb0, rb1, rb2,
                dgs, dgr, xsb, usb, hsb, dgb,
                wsem, lsem, snd, rcv, rs_s, rs_r, dg_s, dg_r, osem, psem, credit):
    dp = lax.axis_index('dp')
    y, x, c = place()
    chip = y * 2 + x
    me = chip * 2 + c
    yp, xp = flip_if(y, c), flip_if(x, 1 - c)
    ys, xs = flip_if(y, 1 - c), flip_if(x, c)
    cp, cs, cd = yp * 2 + xp, ys * 2 + xs, (1 - y) * 2 + (1 - x)

    def dev(yy, xx, cc):
        return (dp, yy, xx * 2 + cc)

    partner, prim, sec = dev(y, x, 1 - c), dev(yp, xp, c), dev(ys, xs, c)

    def rcopy(src, dst, ss, rs, target):
        return pltpu.make_async_remote_copy(src_ref=src, dst_ref=dst, send_sem=ss, recv_sem=rs,
                                            device_id=target, device_id_type=MESH)

    def load(src, dst, sem):
        return pltpu.make_async_copy(src, dst, sem)

    def start_gate_up(e, sl):
        for lo in range(0, D, 256):
            rows = pl.ds(lo, 256)
            load(wg_hbm.at[e, rows], wgu.at[sl, rows, pl.ds(0, F)], wsem.at[sl, 0]).start()
            load(wu_hbm.at[e, rows], wgu.at[sl, rows, pl.ds(F, F)], wsem.at[sl, 1]).start()

    def start_down(e, sl):
        for lo in range(0, F, 176):
            rows = pl.ds(lo, 176)
            load(wd_hbm.at[e, rows], wd.at[sl, rows], wsem.at[sl, 2]).start()

    def wait_gate_up(e, sl):
        load(wg_hbm.at[e], wgu.at[sl, :, pl.ds(0, F)], wsem.at[sl, 0]).wait()
        load(wu_hbm.at[e], wgu.at[sl, :, pl.ds(F, F)], wsem.at[sl, 1]).wait()

    def wait_down(e, sl):
        load(wd_hbm.at[e], wd.at[sl], wsem.at[sl, 2]).wait()

    ins = (load(id_hbm, idall.at[me], lsem.at[0]), load(ga_hbm, gaall.at[me], lsem.at[1]),
           load(x_hbm, xall.at[me], lsem.at[2]), load(dy_hbm, dyall.at[me], lsem.at[3]))
    for cpy in ins:
        cpy.start()

    barrier = pltpu.get_barrier_semaphore()
    others = [lax.rem(me + k, ND) for k in range(1, ND)]
    for t in others:
        pl.semaphore_signal(barrier, inc=1, device_id=(dp, t // 4, lax.rem(t, 4)), device_id_type=MESH)
    pl.semaphore_wait(barrier, ND - 1)

    hw = TD // 2
    bufs = (lambda k: idall.at[k], lambda k: gaall.at[k],
            lambda k: xall.at[k, pl.ds(0, hw)], lambda k: xall.at[k, pl.ds(hw, hw)],
            lambda k: dyall.at[k])
    me_p, me_s, me_d = cp * 2 + c, cs * 2 + c, cd * 2 + c

    def ag_send(st, chunk, k, r, target):
        buf = bufs[st]
        return rcopy(buf(chunk), buf(chunk), snd.at[st, k], rcv.at[st, r], target)

    def ag_wait(st, chunk, r):
        ag_send(st, chunk, 0, r, partner).wait_recv()

    def ag_open(st):
        ag_send(st, me, 0, 0, prim).start()
        ag_send(st, me, 1, 1, sec).start()
        ag_send(st, me, 2, 3, partner).start()

    def ag_first(st):
        ag_wait(st, me_p, 0)
        ag_send(st, me_p, 3, 2, sec).start()
        ag_send(st, me_p, 4, 5, partner).start()

    def ag_second(st):
        ag_wait(st, me_s, 1)
        ag_send(st, me_s, 5, 4, partner).start()

    def ag_diag(st):
        ag_wait(st, me_d, 2)
        ag_send(st, me_d, 6, 6, partner).start()

    def ag_last(st):
        oc = 1 - c
        ag_wait(st, chip * 2 + oc, 3)
        ag_wait(st, cp * 2 + oc, 4)
        ag_wait(st, cs * 2 + oc, 5)
        ag_wait(st, cd * 2 + oc, 6)

    def ag_sent(st):
        for k, (chunk, target) in enumerate(((me, prim), (me, sec), (me, partner), (me_p, sec),
                                             (me_p, partner), (me_s, partner), (me_d, partner))):
            ag_send(st, chunk, k, 0, target).wait_send()

    for st in range(2):
        ins[st].wait()
        ag_open(st)
    ins[2].wait()
    ag_open(2)
    ag_open(3)
    ins[3].wait()
    start_gate_up(0, 0)
    start_down(0, 0)
    for step in (ag_first, ag_second, ag_diag):
        for st in range(2):
            step(st)
    ag_first(2)
    ag_second(2)
    ag_first(3)
    ag_second(3)
    ag_last(0)
    ag_last(1)

    li = lax.broadcasted_iota(jnp.int32, (128, 128), 0)
    lj = lax.broadcasted_iota(jnp.int32, (128, 128), 1)
    upper = jnp.where((li // TD == lj // TD) & (li < lj), 1.0, 0.0).astype(BF16)
    krow = lax.broadcasted_iota(jnp.int32, (2 * E * CAP, 128), 0).astype(F32)
    pbase = (lax.broadcasted_iota(jnp.int32, (1, 128), 1) // TD * (E * CAP)).astype(F32)
    for p in range(4):
        ids = jnp.concatenate([idall[2 * p], idall[2 * p + 1]], axis=1)
        gv = jnp.concatenate([gaall[2 * p], gaall[2 * p + 1]], axis=1)
        sel = jnp.zeros((2 * E * CAP, 128), F32)
        for e in range(E):
            eq = ids == me * E + e
            hit = jnp.sum(jnp.where(eq, 1.0, 0.0), axis=0, keepdims=True)
            gate = jnp.sum(jnp.where(eq, gv, 0.0), axis=0, keepdims=True)
            hit8 = jnp.broadcast_to(hit, (8, 128))
            rank = jnp.where(hit8 > 0.5, dot(hit8.astype(BF16), upper), -1000.0)
            rk[e, :, 128 * p:128 * (p + 1)] = rank
            gt[e, :, 128 * p:128 * (p + 1)] = jnp.broadcast_to(gate, (8, 128))
            sel = jnp.where(rank[0:1, :] + pbase + float(e * CAP) == krow, 1.0, sel)
        psel[p] = sel.astype(BF16)

    tok = lax.broadcasted_iota(jnp.int32, (1, ND * TD), 1)
    slot_base = (tok // TD * CAP).astype(F32)
    slot_row = lax.broadcasted_iota(jnp.int32, (ROWS, ND * TD), 0).astype(F32)

    def slot_mask(e):
        return (rk[e][0:1, :] + slot_base) == slot_row

    def put_rows(e, c0, width, val):
        for s in range(ND):
            oall[s, e, :, c0:c0 + width] = val[s * CAP:(s + 1) * CAP]

    ag_diag(2)
    ag_diag(3)
    start_gate_up(1, 1)
    start_down(1, 1)
    ag_open(4)
    ag_last(2)
    ag_last(3)

    def fwd(e, carry):
        sl = lax.rem(e, 2)
        sel = jnp.where(slot_mask(e), 1.0, 0.0).astype(BF16)

        @pl.when(e > 0)
        def _():
            load(xsb, xs_out.at[e], osem.at[0]).wait()
            load(hsb, hs_out.at[e], osem.at[1]).wait()

        for n in range(4):
            xsb[:, 512 * n:512 * (n + 1)] = dot(sel, xall[:, :, 512 * n:512 * (n + 1)].reshape(ND * TD, 512)).astype(BF16)
        load(xsb, xs_out.at[e], osem.at[0]).start()
        wait_gate_up(e, sl)
        for n in range(6):
            lo, w = 256 * n, 256 if n < 5 else 128
            if w == 256:
                a = dot(xsb[...], wgu[sl, :, lo:lo + w])
                b = dot(xsb[...], wgu[sl, :, F + lo:F + lo + w])
            else:
                rhs = jnp.concatenate([wgu[sl, :, lo:lo + w], wgu[sl, :, F + lo:F + lo + w]], axis=1)
                r = dot(xsb[...], rhs)
                a, b = r[:, :w], r[:, w:]
            ab[e, :, lo:lo + w] = a
            ab[e, :, F + lo:F + lo + w] = b
            hsb[:, lo:lo + w] = (a * jax.nn.sigmoid(a) * b).astype(BF16)
        load(hsb, hs_out.at[e], osem.at[1]).start()

        @pl.when(e < 2)
        def _():
            start_gate_up(e + 2, sl)

        wait_down(e, sl)
        for n in range(8):
            put_rows(e, 256 * n, 256, dot(hsb[...], wd[sl, :, 256 * n:256 * (n + 1)]).astype(BF16))

        @pl.when(e < 2)
        def _():
            start_down(e + 2, sl)

        @pl.when(e == 1)
        def _():
            ag_first(4)

        @pl.when(e == 2)
        def _():
            ag_second(4)
            ag_diag(4)

        return carry

    lax.fori_loop(0, E, fwd, 0)
    load(xsb, xs_out.at[E - 1], osem.at[0]).wait()
    load(hsb, hs_out.at[E - 1], osem.at[1]).wait()
    ag_last(4)

    def combine_y(p, carry):
        lanes = pl.ds(pl.multiple_of(p * 128, 128), 128)
        gates = jnp.zeros((2 * E * CAP, 128), F32)
        for e in range(E):
            hit = rk[e, :, lanes][0:1, :] + pbase + float(e * CAP) == krow
            gates = jnp.where(hit, gt[e, :, lanes][0:1, :], gates)
        g1 = gates.astype(BF16)
        rest = gates - g1.astype(F32)
        g2 = rest.astype(BF16)
        g3 = (rest - g2.astype(F32)).astype(BF16)
        lhs = jnp.concatenate([g1, g2, g3], axis=1)
        for n in range(4):
            cols = slice(512 * n, 512 * (n + 1))
            rhs = oall[pl.ds(2 * p, 2), :, :, cols].reshape(2 * E * CAP, 512)
            r = dot(lhs, rhs, TN)
            r = r[0:128] + (r[128:256] + r[256:384])
            py[0, p, :, cols] = r[0:TD]
            py[1, p, :, cols] = r[TD:]
        return carry

    lax.fori_loop(0, 4, combine_y, 0)

    rs0 = rcopy(py.at[1 - c], rb0, rs_s.at[0], rs_r.at[0], partner)
    rs1a = rcopy(py.at[c, cd], rb1.at[1], rs_s.at[1], rs_r.at[1], prim)
    rs1b = rcopy(py.at[c, cp], rb1.at[0], rs_s.at[2], rs_r.at[2], prim)
    rs2 = rcopy(py.at[c, cs], rb2, rs_s.at[3], rs_r.at[3], sec)
    rs0.start()

    def dx_copy(m):
        cols = pl.ds(512 * m, 512)
        return rcopy(ab.at[:, pl.ds(pl.multiple_of((1 - c) * TD, TD), TD), cols], rb0.at[:, :, cols],
                     rs_s.at[4 + m], rs_r.at[4 + m], partner)

    def combine_dx(m):
        cols = slice(512 * m, 512 * (m + 1))

        def body(p, carry):
            rhs = oall[pl.ds(2 * p, 2), :, :, cols].reshape(2 * E * CAP, 512)
            ab[p, 0:2 * TD, cols] = dot(psel[p], rhs, TN)
            return carry

        lax.fori_loop(0, 4, body, 0)
        dx_copy(m).start()

    def bwd(n, carry):
        e = E - 1 - n
        sl = lax.rem(e, 2)
        mask = slot_mask(e)
        sel = jnp.where(mask, 1.0, 0.0).astype(BF16)
        gcol = jnp.sum(jnp.where(mask, gt[e][0:1, :], 0.0), axis=1, keepdims=True)

        @pl.when(n > 0)
        def _():
            load(usb, us_out.at[e], osem.at[0]).wait()
            load(dgb, dgu_out.at[e], osem.at[1]).wait()

        dgv = jnp.zeros((ROWS, 1), F32)
        for m in range(4):
            c0 = 512 * m
            dye = dot(sel, dyall[:, :, c0:c0 + 512].reshape(ND * TD, 512))
            usb[:, c0:c0 + 512] = (gcol * dye).astype(BF16)
            oe = jnp.concatenate([oall[s, e, :, c0:c0 + 512] for s in range(ND)], axis=0).astype(F32)
            dgv = dgv + jnp.sum(dye * oe, axis=1, keepdims=True)
        dgrow = jnp.sum(jnp.where(mask, dgv, 0.0), axis=0, keepdims=True)
        dgs[e] = jnp.broadcast_to(dgrow, (8, ND * TD))
        load(usb, us_out.at[e], osem.at[0]).start()

        @pl.when(n >= 2)
        def _():
            wait_down(e, sl)

        for lo in range(0, F, 256):
            hi = min(lo + 256, F)
            q = dot(wd[sl, lo:hi, :], usb[...], NT).T
            a = ab[e, :, lo:hi]
            b = ab[e, :, F + lo:F + hi]
            s = jax.nn.sigmoid(a)
            dgb[:, F + lo:F + hi] = (q * a * s).astype(BF16)
            dgb[:, lo:hi] = (q * b * s * (1.0 + a * (1.0 - s))).astype(BF16)
        load(dgb, dgu_out.at[e], osem.at[1]).start()

        @pl.when(n < 2)
        def _():
            start_down(1 - n, sl)

        @pl.when(n == 2)
        def _():
            rs1a.wait_recv()
            py[c, cs] = py[c, cs] + rb1[1]
            rs2.start()

        @pl.when(n >= 2)
        def _():
            wait_gate_up(e, sl)

        for m in range(4):
            dxt = dot(wgu[sl, 512 * m:512 * (m + 1), :], dgb[...], NT)
            put_rows(e, 512 * m, 512, dxt.T.astype(BF16))

        @pl.when(n < 2)
        def _():
            start_gate_up(1 - n, sl)

        @pl.when(n == 0)
        def _():
            rs0.wait()
            py[c] = py[c] + rb0[...]
            rs1a.start()
            rs1b.start()
            pl.semaphore_signal(credit, inc=1, device_id=partner, device_id_type=MESH)

        return carry

    lax.fori_loop(0, E, bwd, 0)
    pl.semaphore_wait(credit, 1)
    for m in range(4):
        combine_dx(m)
    load(usb, us_out.at[0], osem.at[0]).wait()
    load(dgb, dgu_out.at[0], osem.at[1]).wait()

    sends = []
    for i, t in enumerate(others):
        lanes = pl.ds(pl.multiple_of(t // 2 * 128, 128), 128)
        cpy = rcopy(dgs.at[:, :, lanes], dgr.at[me], dg_s.at[i], dg_r.at[me],
                    (dp, t // 4, lax.rem(t, 4)))
        cpy.start()
        sends.append(cpy)
    dgr[me] = dgs[:, :, pl.ds(pl.multiple_of(chip * 128, 128), 128)]

    rs1b.wait_recv()
    rs2.wait_recv()
    y_out[...] = (py[c, chip] + rb1[0] + rb2[...]).astype(BF16)

    own_rows = pl.ds(pl.multiple_of(c * TD, TD), TD)
    dst = ((cp, s1_out.at[0]), (cd, s1_out.at[1]), (chip, own_out), (cs, sec_out))
    parts = []
    for m in range(4):
        dx_copy(m).wait_recv()
        for i, (k, out) in enumerate(dst):
            cols = slice(512 * m, 512 * (m + 1))
            ab[i, 2 * TD:3 * TD, cols] = ab[k, own_rows, cols] + rb0[k, :, cols]
            cpy = load(ab.at[i, pl.ds(2 * TD, TD), pl.ds(512 * m, 512)], out.at[:, pl.ds(512 * m, 512)], psem.at[i, m])
            cpy.start()
            parts.append(cpy)

    for i, t in enumerate(others):
        rcopy(dgs.at[:, :, pl.ds(0, 128)], dgr.at[t], dg_s.at[i], dg_r.at[t], partner).wait_recv()
    ids = idall[me]
    acc = jnp.zeros((K, TD), F32)
    for t in range(ND):
        for e in range(E):
            row = dgr[t, e][0:1, :]
            row = jnp.where(c == 0, row[:, 0:TD], row[:, TD:2 * TD])
            acc = acc + jnp.where(ids == t * E + e, row, 0.0)
    dgt_out[...] = acc

    for m in range(4):
        dx_copy(m).wait_send()
    rs1a.wait_send()
    rs1b.wait_send()
    rs2.wait_send()
    for st in range(5):
        ag_sent(st)
    for cpy in sends:
        cpy.wait_send()
    for cpy in parts:
        cpy.wait()


def run_main(tok, dy, idt, gat, wg, wu, wd):
    anys = pl.BlockSpec(memory_space=pl.ANY)
    vm = pl.BlockSpec(memory_space=pltpu.VMEM)
    V = pltpu.VMEM
    S = pltpu.SemaphoreType.DMA
    flops = 2 * E * ROWS * D * F * 6
    return pl.pallas_call(
        main_kernel,
        name='moe_main',
        out_shape=(jax.ShapeDtypeStruct((TD, D), BF16), jax.ShapeDtypeStruct((K, TD), F32),
                   jax.ShapeDtypeStruct((2, TD, D), F32), jax.ShapeDtypeStruct((TD, D), F32),
                   jax.ShapeDtypeStruct((TD, D), F32),
                   jax.ShapeDtypeStruct((E, ROWS, D), BF16), jax.ShapeDtypeStruct((E, ROWS, D), BF16),
                   jax.ShapeDtypeStruct((E, ROWS, F), BF16), jax.ShapeDtypeStruct((E, ROWS, 2 * F), BF16)),
        in_specs=[anys] * 7,
        out_specs=(vm, vm) + (anys,) * 7,
        scratch_shapes=[
            V((2, D, 2 * F), BF16), V((2, F, D), BF16),
            V((ND, TD, D), BF16), V((ND, TD, D), BF16), V((ND, K, TD), jnp.int32), V((ND, K, TD), F32),
            V((E, 8, ND * TD), F32), V((E, 8, ND * TD), F32), V((4, 2 * E * CAP, 128), BF16),
            V((E, ROWS, 2 * F), F32), V((ND, E, CAP, D), BF16),
            V((2, 4, TD, D), F32), V((4, TD, D), F32), V((2, TD, D), F32), V((TD, D), F32),
            V((E, 8, ND * TD), F32), V((ND, E, 8, 128), F32),
            V((ROWS, D), BF16), V((ROWS, D), BF16), V((ROWS, F), BF16), V((ROWS, 2 * F), BF16),
            S((2, 3)), S((4,)), S((5, 7)), S((5, 7)), S((8,)), S((8,)), S((7,)), S((ND,)), S((2,)), S((4, 4)),
            pltpu.SemaphoreType.REGULAR,
        ],
        compiler_params=pltpu.CompilerParams(collective_id=0, has_side_effects=True,
                                             vmem_limit_bytes=67043328),
        cost_estimate=pl.CostEstimate(flops=flops, bytes_accessed=120_000_000, transcendentals=0),
    )(tok, dy, idt, gat, wg, wu, wd)


RING = 4


def ring_loop(steps, ring, outs, compute):
    def body(i, carry):
        slot = lax.rem(i, ring)

        @pl.when(i >= ring)
        def _():
            for cpy in outs(i - ring, slot):
                cpy.wait()

        compute(i, slot)
        for cpy in outs(i, slot):
            cpy.start()
        return carry

    lax.fori_loop(0, steps, body, 0)
    for k in range(ring):
        i = steps - ring + k
        for cpy in outs(i, i % ring):
            cpy.wait()


def gate_up_kernel(x_hbm, g_hbm, og_hbm, ou_hbm, x_v, g_v, og_v, ou_v, isem, osem):
    def ins(e):
        return (pltpu.make_async_copy(x_hbm.at[e], x_v.at[e], isem.at[e, 0]),
                pltpu.make_async_copy(g_hbm.at[e], g_v.at[e], isem.at[e, 1]))

    for e in range(E):
        for cpy in ins(e):
            cpy.start()

    def outs(i, slot):
        rows = pl.ds(pl.multiple_of(lax.rem(i, 4) * 512, 512), 512)
        return (pltpu.make_async_copy(og_v.at[slot], og_hbm.at[i // 4, rows], osem.at[slot, 0]),
                pltpu.make_async_copy(ou_v.at[slot], ou_hbm.at[i // 4, rows], osem.at[slot, 1]))

    def compute(i, slot):
        e = i // 4

        @pl.when(lax.rem(i, 4) == 0)
        def _():
            for cpy in ins(e):
                cpy.wait()

        cols = pl.ds(pl.multiple_of(lax.rem(i, 4) * 512, 512), 512)
        r = dot(x_v[e, :, cols], g_v[e], TN)
        og_v[slot] = r[:, :F].astype(BF16)
        ou_v[slot] = r[:, F:].astype(BF16)

    ring_loop(4 * E, RING, outs, compute)


def run_gate_up(xs, dgu):
    anys = pl.BlockSpec(memory_space=pl.ANY)
    V = pltpu.VMEM
    return pl.pallas_call(
        gate_up_kernel, name='moe_dw_gate_up',
        in_specs=[anys, anys], out_specs=(anys, anys),
        out_shape=(jax.ShapeDtypeStruct((E, D, F), BF16),) * 2,
        scratch_shapes=[V((E, ROWS, D), BF16), V((E, ROWS, 2 * F), BF16),
                        V((RING, 512, F), BF16), V((RING, 512, F), BF16),
                        pltpu.SemaphoreType.DMA((E, 2)), pltpu.SemaphoreType.DMA((RING, 2))],
        compiler_params=pltpu.CompilerParams(vmem_limit_bytes=67043328),
        cost_estimate=pl.CostEstimate(flops=4 * E * ROWS * D * F, bytes_accessed=55_000_000, transcendentals=0),
    )(xs, dgu)


def down_kernel(h_hbm, u_hbm, o_hbm, h_v, u_v, ht_v, o_v, isem, osem):
    def ins(e):
        return (pltpu.make_async_copy(h_hbm.at[e], h_v.at[e], isem.at[e, 0]),
                pltpu.make_async_copy(u_hbm.at[e], u_v.at[e], isem.at[e, 1]))

    for e in range(E):
        for cpy in ins(e):
            cpy.start()

    def cols(i):
        return pl.ds(pl.multiple_of(lax.rem(i, 4) * 512, 512), 512)

    def outs(i, slot):
        return (pltpu.make_async_copy(o_v.at[slot], o_hbm.at[i // 4, :, cols(i)], osem.at[slot]),)

    def compute(i, slot):
        e = i // 4

        @pl.when(lax.rem(i, 4) == 0)
        def _():
            for cpy in ins(e):
                cpy.wait()
            ht_v[...] = h_v[e].T

        o_v[slot] = dot(ht_v[...], u_v[e, :, cols(i)]).astype(BF16)

    ring_loop(4 * E, RING, outs, compute)


def run_down(hs, us):
    anys = pl.BlockSpec(memory_space=pl.ANY)
    V = pltpu.VMEM
    return pl.pallas_call(
        down_kernel, name='moe_dw_down',
        in_specs=[anys, anys], out_specs=anys,
        out_shape=jax.ShapeDtypeStruct((E, F, D), BF16),
        scratch_shapes=[V((E, ROWS, F), BF16), V((E, ROWS, D), BF16), V((F, ROWS), BF16), V((RING, F, 512), BF16),
                        pltpu.SemaphoreType.DMA((E, 2)), pltpu.SemaphoreType.DMA((RING,))],
        compiler_params=pltpu.CompilerParams(vmem_limit_bytes=67043328),
        cost_estimate=pl.CostEstimate(flops=2 * E * ROWS * D * F, bytes_accessed=28_000_000, transcendentals=0),
    )(hs, us)


def exchange_pairs(kind):
    pairs = []
    for y in range(2):
        for x in range(2):
            for c in range(2):
                if (kind == 'prim') == (c == 0):
                    t = (y, 1 - x, c)
                else:
                    t = (1 - y, x, c)
                pairs.append((y * 4 + x * 2 + c, t[0] * 4 + t[1] * 2 + t[2]))
    return pairs


def solution(mesh):
    tok_spec = P(('dp', 'ei', 'eo'))
    exp_spec = P(('ei', 'eo'))

    def device_step(tok, idx, gate, wg, wu, wd, dy):
        layer_out, dgt, s1, own, second, xs, us, hs, dgu = run_main(tok, dy, idx.T, gate.T, wg, wu, wd)
        perm = functools.partial(lax.ppermute, axis_name=('ei', 'eo'))
        r1 = perm(s1, perm=exchange_pairs('prim'))
        g_gate, g_up = run_gate_up(xs, dgu)
        g_down = run_down(hs, us)
        r2 = perm(second + r1[1], perm=exchange_pairs('sec'))
        grad_tok = (own + r1[0] + r2).astype(BF16)
        dgk = dgt.T
        return layer_out, grad_tok, dgk, g_gate, g_up, g_down

    return jax.shard_map(device_step, mesh=mesh,
                         in_specs=(tok_spec, tok_spec, tok_spec, exp_spec, exp_spec, exp_spec, tok_spec),
                         out_specs=(tok_spec, tok_spec, tok_spec, tok_spec, tok_spec, tok_spec), check_vma=False)
```

```python
import functools

import jax
import jax.numpy as jnp
from jax import lax
from jax.experimental import pallas as pl
from jax.experimental.pallas import tpu as pltpu
from jax.sharding import PartitionSpec as P


F32 = jnp.float32
BF16 = jnp.bfloat16
MESH = pl.DeviceIdType.MESH

TD = 64
D = 2048
F = 1408
K = 6
E = 4
CAP = 24
ND = 8
ROWS = ND * CAP

NT = (((1,), (1,)), ((), ()))
TN = (((0,), (0,)), ((), ()))


def dot(a, b, dims=None):
    if dims is None:
        return jnp.dot(a, b, preferred_element_type=F32)
    return lax.dot_general(a, b, dims, preferred_element_type=F32)


def place():
    y = lax.axis_index('ei')
    o = lax.axis_index('eo')
    x = o // 2
    c = o % 2
    return y, x, c


def flip_if(v, f):
    return v + f - 2 * v * f


def main_kernel(x_hbm, dy_hbm, id_hbm, ga_hbm, wg_hbm, wu_hbm, wd_hbm,
                y_out, dgt_out, s1_out, own_out, sec_out, xs_out, us_out, hs_out, dgu_out,
                wgu, wd, xall, dyall, idall, gaall, rk, gt, psel, ab, oall, py, rb0, rb1, rb2,
                dgs, dgr, xsb, usb, hsb, dgb,
                wsem, lsem, snd, rcv, rs_s, rs_r, dg_s, dg_r, osem, psem, credit):
    dp = lax.axis_index('dp')
    y, x, c = place()
    chip = y * 2 + x
    me = chip * 2 + c
    yp, xp = flip_if(y, c), flip_if(x, 1 - c)
    ys, xs = flip_if(y, 1 - c), flip_if(x, c)
    cp, cs, cd = yp * 2 + xp, ys * 2 + xs, (1 - y) * 2 + (1 - x)

    def dev(yy, xx, cc):
        return (dp, yy, xx * 2 + cc)

    partner, prim, sec = dev(y, x, 1 - c), dev(yp, xp, c), dev(ys, xs, c)

    def rcopy(src, dst, ss, rs, target):
        return pltpu.make_async_remote_copy(src_ref=src, dst_ref=dst, send_sem=ss, recv_sem=rs,
                                            device_id=target, device_id_type=MESH)

    def load(src, dst, sem):
        return pltpu.make_async_copy(src, dst, sem)

    def start_gate_up(e, sl):
        for lo in range(0, D, 256):
            rows = pl.ds(lo, 256)
            load(wg_hbm.at[e, rows], wgu.at[sl, rows, pl.ds(0, F)], wsem.at[sl, 0]).start()
            load(wu_hbm.at[e, rows], wgu.at[sl, rows, pl.ds(F, F)], wsem.at[sl, 1]).start()

    def start_down(e, sl):
        for lo in range(0, F, 176):
            rows = pl.ds(lo, 176)
            load(wd_hbm.at[e, rows], wd.at[sl, rows], wsem.at[sl, 2]).start()

    def wait_gate_up(e, sl):
        load(wg_hbm.at[e], wgu.at[sl, :, pl.ds(0, F)], wsem.at[sl, 0]).wait()
        load(wu_hbm.at[e], wgu.at[sl, :, pl.ds(F, F)], wsem.at[sl, 1]).wait()

    def wait_down(e, sl):
        load(wd_hbm.at[e], wd.at[sl], wsem.at[sl, 2]).wait()

    ins = (load(id_hbm, idall.at[me], lsem.at[0]), load(ga_hbm, gaall.at[me], lsem.at[1]),
           load(x_hbm, xall.at[me], lsem.at[2]), load(dy_hbm, dyall.at[me], lsem.at[3]))
    for cpy in ins:
        cpy.start()

    barrier = pltpu.get_barrier_semaphore()
    others = [lax.rem(me + k, ND) for k in range(1, ND)]
    for t in others:
        pl.semaphore_signal(barrier, inc=1, device_id=(dp, t // 4, lax.rem(t, 4)), device_id_type=MESH)
    pl.semaphore_wait(barrier, ND - 1)

    hw = TD // 2
    bufs = (lambda k: idall.at[k], lambda k: gaall.at[k],
            lambda k: xall.at[k, pl.ds(0, hw)], lambda k: xall.at[k, pl.ds(hw, hw)],
            lambda k: dyall.at[k])
    me_p, me_s, me_d = cp * 2 + c, cs * 2 + c, cd * 2 + c

    def ag_send(st, chunk, k, r, target):
        buf = bufs[st]
        return rcopy(buf(chunk), buf(chunk), snd.at[st, k], rcv.at[st, r], target)

    def ag_wait(st, chunk, r):
        ag_send(st, chunk, 0, r, partner).wait_recv()

    def ag_open(st):
        ag_send(st, me, 0, 0, prim).start()
        ag_send(st, me, 1, 1, sec).start()
        ag_send(st, me, 2, 3, partner).start()

    def ag_first(st):
        ag_wait(st, me_p, 0)
        ag_send(st, me_p, 3, 2, sec).start()
        ag_send(st, me_p, 4, 5, partner).start()

    def ag_second(st):
        ag_wait(st, me_s, 1)
        ag_send(st, me_s, 5, 4, partner).start()

    def ag_diag(st):
        ag_wait(st, me_d, 2)
        ag_send(st, me_d, 6, 6, partner).start()

    def ag_last(st):
        oc = 1 - c
        ag_wait(st, chip * 2 + oc, 3)
        ag_wait(st, cp * 2 + oc, 4)
        ag_wait(st, cs * 2 + oc, 5)
        ag_wait(st, cd * 2 + oc, 6)

    def ag_sent(st):
        for k, (chunk, target) in enumerate(((me, prim), (me, sec), (me, partner), (me_p, sec),
                                             (me_p, partner), (me_s, partner), (me_d, partner))):
            ag_send(st, chunk, k, 0, target).wait_send()

    for st in range(2):
        ins[st].wait()
        ag_open(st)
    ins[2].wait()
    ag_open(2)
    ag_open(3)
    ins[3].wait()
    start_gate_up(0, 0)
    start_down(0, 0)
    for step in (ag_first, ag_second, ag_diag):
        for st in range(2):
            step(st)
    ag_first(2)
    ag_second(2)
    ag_first(3)
    ag_second(3)
    ag_last(0)
    ag_last(1)

    li = lax.broadcasted_iota(jnp.int32, (128, 128), 0)
    lj = lax.broadcasted_iota(jnp.int32, (128, 128), 1)
    upper = jnp.where((li // TD == lj // TD) & (li < lj), 1.0, 0.0).astype(BF16)
    krow = lax.broadcasted_iota(jnp.int32, (2 * E * CAP, 128), 0).astype(F32)
    pbase = (lax.broadcasted_iota(jnp.int32, (1, 128), 1) // TD * (E * CAP)).astype(F32)
    for p in range(4):
        ids = jnp.concatenate([idall[2 * p], idall[2 * p + 1]], axis=1)
        gv = jnp.concatenate([gaall[2 * p], gaall[2 * p + 1]], axis=1)
        sel = jnp.zeros((2 * E * CAP, 128), F32)
        for e in range(E):
            eq = ids == me * E + e
            hit = jnp.sum(jnp.where(eq, 1.0, 0.0), axis=0, keepdims=True)
            gate = jnp.sum(jnp.where(eq, gv, 0.0), axis=0, keepdims=True)
            hit8 = jnp.broadcast_to(hit, (8, 128))
            rank = jnp.where(hit8 > 0.5, dot(hit8.astype(BF16), upper), -1000.0)
            rk[e, :, 128 * p:128 * (p + 1)] = rank
            gt[e, :, 128 * p:128 * (p + 1)] = jnp.broadcast_to(gate, (8, 128))
            sel = jnp.where(rank[0:1, :] + pbase + float(e * CAP) == krow, 1.0, sel)
        psel[p] = sel.astype(BF16)

    tok = lax.broadcasted_iota(jnp.int32, (1, ND * TD), 1)
    slot_base = (tok // TD * CAP).astype(F32)
    slot_row = lax.broadcasted_iota(jnp.int32, (ROWS, ND * TD), 0).astype(F32)

    def slot_mask(e):
        return (rk[e][0:1, :] + slot_base) == slot_row

    def put_rows(e, c0, width, val):
        for s in range(ND):
            oall[s, e, :, c0:c0 + width] = val[s * CAP:(s + 1) * CAP]

    ag_diag(2)
    ag_diag(3)
    start_gate_up(1, 1)
    start_down(1, 1)
    ag_open(4)
    ag_last(2)
    ag_last(3)

    def fwd(e, carry):
        sl = lax.rem(e, 2)
        sel = jnp.where(slot_mask(e), 1.0, 0.0).astype(BF16)

        @pl.when(e > 0)
        def _():
            load(xsb, xs_out.at[e], osem.at[0]).wait()
            load(hsb, hs_out.at[e], osem.at[1]).wait()

        for n in range(4):
            xsb[:, 512 * n:512 * (n + 1)] = dot(sel, xall[:, :, 512 * n:512 * (n + 1)].reshape(ND * TD, 512)).astype(BF16)
        load(xsb, xs_out.at[e], osem.at[0]).start()
        wait_gate_up(e, sl)
        for n in range(6):
            lo, w = 256 * n, 256 if n < 5 else 128
            if w == 256:
                a = dot(xsb[...], wgu[sl, :, lo:lo + w])
                b = dot(xsb[...], wgu[sl, :, F + lo:F + lo + w])
            else:
                rhs = jnp.concatenate([wgu[sl, :, lo:lo + w], wgu[sl, :, F + lo:F + lo + w]], axis=1)
                r = dot(xsb[...], rhs)
                a, b = r[:, :w], r[:, w:]
            ab[e, :, lo:lo + w] = a
            ab[e, :, F + lo:F + lo + w] = b
            hsb[:, lo:lo + w] = (a * jax.nn.sigmoid(a) * b).astype(BF16)
        load(hsb, hs_out.at[e], osem.at[1]).start()

        @pl.when(e < 2)
        def _():
            start_gate_up(e + 2, sl)

        wait_down(e, sl)
        for n in range(8):
            put_rows(e, 256 * n, 256, dot(hsb[...], wd[sl, :, 256 * n:256 * (n + 1)]).astype(BF16))

        @pl.when(e < 2)
        def _():
            start_down(e + 2, sl)

        @pl.when(e == 1)
        def _():
            ag_first(4)

        @pl.when(e == 2)
        def _():
            ag_second(4)
            ag_diag(4)

        return carry

    lax.fori_loop(0, E, fwd, 0)
    load(xsb, xs_out.at[E - 1], osem.at[0]).wait()
    load(hsb, hs_out.at[E - 1], osem.at[1]).wait()
    ag_last(4)

    def combine_y(p, carry):
        lanes = pl.ds(pl.multiple_of(p * 128, 128), 128)
        gates = jnp.zeros((2 * E * CAP, 128), F32)
        for e in range(E):
            hit = rk[e, :, lanes][0:1, :] + pbase + float(e * CAP) == krow
            gates = jnp.where(hit, gt[e, :, lanes][0:1, :], gates)
        g1 = gates.astype(BF16)
        rest = gates - g1.astype(F32)
        g2 = rest.astype(BF16)
        g3 = (rest - g2.astype(F32)).astype(BF16)
        lhs = jnp.concatenate([g1, g2, g3], axis=1)
        for n in range(4):
            cols = slice(512 * n, 512 * (n + 1))
            rhs = oall[pl.ds(2 * p, 2), :, :, cols].reshape(2 * E * CAP, 512)
            r = dot(lhs, rhs, TN)
            r = r[0:128] + (r[128:256] + r[256:384])
            py[0, p, :, cols] = r[0:TD]
            py[1, p, :, cols] = r[TD:]
        return carry

    lax.fori_loop(0, 4, combine_y, 0)

    rs0 = rcopy(py.at[1 - c], rb0, rs_s.at[0], rs_r.at[0], partner)
    rs1a = rcopy(py.at[c, cd], rb1.at[1], rs_s.at[1], rs_r.at[1], prim)
    rs1b = rcopy(py.at[c, cp], rb1.at[0], rs_s.at[2], rs_r.at[2], prim)
    rs2 = rcopy(py.at[c, cs], rb2, rs_s.at[3], rs_r.at[3], sec)
    rs0.start()

    def dx_copy(m):
        cols = pl.ds(512 * m, 512)
        return rcopy(ab.at[:, pl.ds(pl.multiple_of((1 - c) * TD, TD), TD), cols], rb0.at[:, :, cols],
                     rs_s.at[4 + m], rs_r.at[4 + m], partner)

    def combine_dx(m):
        cols = slice(512 * m, 512 * (m + 1))

        def body(p, carry):
            rhs = oall[pl.ds(2 * p, 2), :, :, cols].reshape(2 * E * CAP, 512)
            ab[p, 0:2 * TD, cols] = dot(psel[p], rhs, TN)
            return carry

        lax.fori_loop(0, 4, body, 0)
        dx_copy(m).start()

    def bwd(n, carry):
        e = E - 1 - n
        sl = lax.rem(e, 2)
        mask = slot_mask(e)
        sel = jnp.where(mask, 1.0, 0.0).astype(BF16)
        gcol = jnp.sum(jnp.where(mask, gt[e][0:1, :], 0.0), axis=1, keepdims=True)

        @pl.when(n > 0)
        def _():
            load(usb, us_out.at[e], osem.at[0]).wait()
            load(dgb, dgu_out.at[e], osem.at[1]).wait()

        dgv = jnp.zeros((ROWS, 1), F32)
        for m in range(4):
            c0 = 512 * m
            dye = dot(sel, dyall[:, :, c0:c0 + 512].reshape(ND * TD, 512))
            usb[:, c0:c0 + 512] = (gcol * dye).astype(BF16)
            oe = jnp.concatenate([oall[s, e, :, c0:c0 + 512] for s in range(ND)], axis=0).astype(F32)
            dgv = dgv + jnp.sum(dye * oe, axis=1, keepdims=True)
        dgrow = jnp.sum(jnp.where(mask, dgv, 0.0), axis=0, keepdims=True)
        dgs[e] = jnp.broadcast_to(dgrow, (8, ND * TD))
        load(usb, us_out.at[e], osem.at[0]).start()

        @pl.when(n >= 2)
        def _():
            wait_down(e, sl)

        for lo in range(0, F, 256):
            hi = min(lo + 256, F)
            q = dot(wd[sl, lo:hi, :], usb[...], NT).T
            a = ab[e, :, lo:hi]
            b = ab[e, :, F + lo:F + hi]
            s = jax.nn.sigmoid(a)
            dgb[:, F + lo:F + hi] = (q * a * s).astype(BF16)
            dgb[:, lo:hi] = (q * b * s * (1.0 + a * (1.0 - s))).astype(BF16)
        load(dgb, dgu_out.at[e], osem.at[1]).start()

        @pl.when(n < 2)
        def _():
            start_down(1 - n, sl)

        @pl.when(n == 2)
        def _():
            rs1a.wait_recv()
            py[c, cs] = py[c, cs] + rb1[1]
            rs2.start()

        @pl.when(n >= 2)
        def _():
            wait_gate_up(e, sl)

        for m in range(4):
            dxt = dot(wgu[sl, 512 * m:512 * (m + 1), :], dgb[...], NT)
            put_rows(e, 512 * m, 512, dxt.T.astype(BF16))

        @pl.when(n < 2)
        def _():
            start_gate_up(1 - n, sl)

        @pl.when(n == 0)
        def _():
            rs0.wait()
            py[c] = py[c] + rb0[...]
            rs1a.start()
            rs1b.start()
            pl.semaphore_signal(credit, inc=1, device_id=partner, device_id_type=MESH)

        return carry

    lax.fori_loop(0, E, bwd, 0)
    pl.semaphore_wait(credit, 1)
    for m in range(4):
        combine_dx(m)
    load(usb, us_out.at[0], osem.at[0]).wait()
    load(dgb, dgu_out.at[0], osem.at[1]).wait()

    sends = []
    for i, t in enumerate(others):
        lanes = pl.ds(pl.multiple_of(t // 2 * 128, 128), 128)
        cpy = rcopy(dgs.at[:, :, lanes], dgr.at[me], dg_s.at[i], dg_r.at[me],
                    (dp, t // 4, lax.rem(t, 4)))
        cpy.start()
        sends.append(cpy)
    dgr[me] = dgs[:, :, pl.ds(pl.multiple_of(chip * 128, 128), 128)]

    rs1b.wait_recv()
    rs2.wait_recv()
    y_out[...] = (py[c, chip] + rb1[0] + rb2[...]).astype(BF16)

    own_rows = pl.ds(pl.multiple_of(c * TD, TD), TD)
    dst = ((cp, s1_out.at[0]), (cd, s1_out.at[1]), (chip, own_out), (cs, sec_out))
    parts = []
    for m in range(4):
        dx_copy(m).wait_recv()
        for i, (k, out) in enumerate(dst):
            cols = slice(512 * m, 512 * (m + 1))
            ab[i, 2 * TD:3 * TD, cols] = ab[k, own_rows, cols] + rb0[k, :, cols]
            cpy = load(ab.at[i, pl.ds(2 * TD, TD), pl.ds(512 * m, 512)], out.at[:, pl.ds(512 * m, 512)], psem.at[i, m])
            cpy.start()
            parts.append(cpy)

    for i, t in enumerate(others):
        rcopy(dgs.at[:, :, pl.ds(0, 128)], dgr.at[t], dg_s.at[i], dg_r.at[t], partner).wait_recv()
    ids = idall[me]
    acc = jnp.zeros((K, TD), F32)
    for t in range(ND):
        for e in range(E):
            row = dgr[t, e][0:1, :]
            row = jnp.where(c == 0, row[:, 0:TD], row[:, TD:2 * TD])
            acc = acc + jnp.where(ids == t * E + e, row, 0.0)
    dgt_out[...] = acc

    for m in range(4):
        dx_copy(m).wait_send()
    rs1a.wait_send()
    rs1b.wait_send()
    rs2.wait_send()
    for st in range(5):
        ag_sent(st)
    for cpy in sends:
        cpy.wait_send()
    for cpy in parts:
        cpy.wait()


def run_main(tok, dy, idt, gat, wg, wu, wd):
    anys = pl.BlockSpec(memory_space=pl.ANY)
    vm = pl.BlockSpec(memory_space=pltpu.VMEM)
    V = pltpu.VMEM
    S = pltpu.SemaphoreType.DMA
    flops = 2 * E * ROWS * D * F * 6
    return pl.pallas_call(
        main_kernel,
        name='moe_main',
        out_shape=(jax.ShapeDtypeStruct((TD, D), BF16), jax.ShapeDtypeStruct((K, TD), F32),
                   jax.ShapeDtypeStruct((2, TD, D), F32), jax.ShapeDtypeStruct((TD, D), F32),
                   jax.ShapeDtypeStruct((TD, D), F32),
                   jax.ShapeDtypeStruct((E, ROWS, D), BF16), jax.ShapeDtypeStruct((E, ROWS, D), BF16),
                   jax.ShapeDtypeStruct((E, ROWS, F), BF16), jax.ShapeDtypeStruct((E, ROWS, 2 * F), BF16)),
        in_specs=[anys] * 7,
        out_specs=(vm, vm) + (anys,) * 7,
        scratch_shapes=[
            V((2, D, 2 * F), BF16), V((2, F, D), BF16),
            V((ND, TD, D), BF16), V((ND, TD, D), BF16), V((ND, K, TD), jnp.int32), V((ND, K, TD), F32),
            V((E, 8, ND * TD), F32), V((E, 8, ND * TD), F32), V((4, 2 * E * CAP, 128), BF16),
            V((E, ROWS, 2 * F), F32), V((ND, E, CAP, D), BF16),
            V((2, 4, TD, D), F32), V((4, TD, D), F32), V((2, TD, D), F32), V((TD, D), F32),
            V((E, 8, ND * TD), F32), V((ND, E, 8, 128), F32),
            V((ROWS, D), BF16), V((ROWS, D), BF16), V((ROWS, F), BF16), V((ROWS, 2 * F), BF16),
            S((2, 3)), S((4,)), S((5, 7)), S((5, 7)), S((8,)), S((8,)), S((7,)), S((ND,)), S((2,)), S((4, 4)),
            pltpu.SemaphoreType.REGULAR,
        ],
        compiler_params=pltpu.CompilerParams(collective_id=0, has_side_effects=True,
                                             vmem_limit_bytes=67043328),
        cost_estimate=pl.CostEstimate(flops=flops, bytes_accessed=120_000_000, transcendentals=0),
    )(tok, dy, idt, gat, wg, wu, wd)


RING = 4


def ring_loop(steps, ring, outs, compute):
    def body(i, carry):
        slot = lax.rem(i, ring)

        @pl.when(i >= ring)
        def _():
            for cpy in outs(i - ring, slot):
                cpy.wait()

        compute(i, slot)
        for cpy in outs(i, slot):
            cpy.start()
        return carry

    lax.fori_loop(0, steps, body, 0)
    for k in range(ring):
        i = steps - ring + k
        for cpy in outs(i, i % ring):
            cpy.wait()


def gate_up_kernel(x_hbm, g_hbm, y_hbm, dg_hbm, og_hbm, ou_hbm, oy_hbm, odg_hbm,
                   x_v, g_v, og_v, ou_v, y_v, dg_v, isem, osem, psem):
    through = ((y_hbm, y_v, oy_hbm), (dg_hbm, dg_v, odg_hbm))

    def ins(e):
        return (pltpu.make_async_copy(x_hbm.at[e], x_v.at[e], isem.at[e, 0]),
                pltpu.make_async_copy(g_hbm.at[e], g_v.at[e], isem.at[e, 1]))

    for e in range(E):
        for cpy in ins(e):
            cpy.start()

    def outs(i, slot):
        rows = pl.ds(pl.multiple_of(lax.rem(i, 4) * 512, 512), 512)
        return (pltpu.make_async_copy(og_v.at[slot], og_hbm.at[i // 4, rows], osem.at[slot, 0]),
                pltpu.make_async_copy(ou_v.at[slot], ou_hbm.at[i // 4, rows], osem.at[slot, 1]))

    def compute(i, slot):
        e = i // 4

        @pl.when(lax.rem(i, 4) == 0)
        def _():
            for cpy in ins(e):
                cpy.wait()

        @pl.when(i == 4)
        def _():
            for k, (src, mid, _) in enumerate(through):
                pltpu.make_async_copy(src, mid, psem.at[k, 0]).start()

        @pl.when(i == 8)
        def _():
            for k, (src, mid, dst) in enumerate(through):
                pltpu.make_async_copy(src, mid, psem.at[k, 0]).wait()
                pltpu.make_async_copy(mid, dst, psem.at[k, 1]).start()

        cols = pl.ds(pl.multiple_of(lax.rem(i, 4) * 512, 512), 512)
        r = dot(x_v[e, :, cols], g_v[e], TN)
        og_v[slot] = r[:, :F].astype(BF16)
        ou_v[slot] = r[:, F:].astype(BF16)

    ring_loop(4 * E, RING, outs, compute)
    for k, (_, mid, dst) in enumerate(through):
        pltpu.make_async_copy(mid, dst, psem.at[k, 1]).wait()


def run_gate_up(xs, dgu, y, dgt):
    anys = pl.BlockSpec(memory_space=pl.ANY)
    V = pltpu.VMEM
    return pl.pallas_call(
        gate_up_kernel, name='moe_dw_gate_up',
        in_specs=[anys] * 4, out_specs=(anys,) * 4,
        out_shape=(jax.ShapeDtypeStruct((E, D, F), BF16),) * 2
        + (jax.ShapeDtypeStruct((TD, D), BF16), jax.ShapeDtypeStruct((K, TD), F32)),
        scratch_shapes=[V((E, ROWS, D), BF16), V((E, ROWS, 2 * F), BF16),
                        V((RING, 512, F), BF16), V((RING, 512, F), BF16), V((TD, D), BF16), V((K, TD), F32),
                        pltpu.SemaphoreType.DMA((E, 2)), pltpu.SemaphoreType.DMA((RING, 2)),
                        pltpu.SemaphoreType.DMA((2, 2))],
        compiler_params=pltpu.CompilerParams(vmem_limit_bytes=67043328),
        cost_estimate=pl.CostEstimate(flops=4 * E * ROWS * D * F, bytes_accessed=55_000_000, transcendentals=0),
    )(xs, dgu, y, dgt)


def down_kernel(h_hbm, u_hbm, o_hbm, h_v, u_v, ht_v, o_v, isem, osem):
    def ins(e):
        return (pltpu.make_async_copy(h_hbm.at[e], h_v.at[e], isem.at[e, 0]),
                pltpu.make_async_copy(u_hbm.at[e], u_v.at[e], isem.at[e, 1]))

    for e in range(E):
        for cpy in ins(e):
            cpy.start()

    def cols(i):
        return pl.ds(pl.multiple_of(lax.rem(i, 2) * 1024, 1024), 1024)

    def outs(i, slot):
        halves = []
        for k in range(2):
            rows = pl.ds(704 * k, 704)
            halves.append(pltpu.make_async_copy(o_v.at[slot, rows], o_hbm.at[i // 2, rows, cols(i)], osem.at[slot, k]))
        return halves

    def compute(i, slot):
        e = i // 2

        @pl.when(lax.rem(i, 2) == 0)
        def _():
            for cpy in ins(e):
                cpy.wait()
            ht_v[...] = h_v[e].T

        o_v[slot] = dot(ht_v[...], u_v[e, :, cols(i)]).astype(BF16)

    ring_loop(2 * E, RING, outs, compute)


def run_down(hs, us):
    anys = pl.BlockSpec(memory_space=pl.ANY)
    V = pltpu.VMEM
    return pl.pallas_call(
        down_kernel, name='moe_dw_down',
        in_specs=[anys, anys], out_specs=anys,
        out_shape=jax.ShapeDtypeStruct((E, F, D), BF16),
        scratch_shapes=[V((E, ROWS, F), BF16), V((E, ROWS, D), BF16), V((F, ROWS), BF16), V((RING, F, 1024), BF16),
                        pltpu.SemaphoreType.DMA((E, 2)), pltpu.SemaphoreType.DMA((RING, 2))],
        compiler_params=pltpu.CompilerParams(vmem_limit_bytes=67043328),
        cost_estimate=pl.CostEstimate(flops=2 * E * ROWS * D * F, bytes_accessed=28_000_000, transcendentals=0),
    )(hs, us)


def exchange_pairs(kind):
    pairs = []
    for y in range(2):
        for x in range(2):
            for c in range(2):
                if (kind == 'prim') == (c == 0):
                    t = (y, 1 - x, c)
                else:
                    t = (1 - y, x, c)
                pairs.append((y * 4 + x * 2 + c, t[0] * 4 + t[1] * 2 + t[2]))
    return pairs


def solution(mesh):
    tok_spec = P(('dp', 'ei', 'eo'))
    exp_spec = P(('ei', 'eo'))

    def device_step(tok, idx, gate, wg, wu, wd, dy):
        layer_out, dgt, s1, own, second, xs, us, hs, dgu = run_main(tok, dy, idx.T, gate.T, wg, wu, wd)
        perm = functools.partial(lax.ppermute, axis_name=('ei', 'eo'))
        r1 = perm(s1, perm=exchange_pairs('prim'))
        g_gate, g_up, layer_out, dgt = run_gate_up(xs, dgu, layer_out, dgt)
        g_down = run_down(hs, us)
        r2 = perm(second + r1[1], perm=exchange_pairs('sec'))
        grad_tok = (own + r1[0] + r2).astype(BF16)
        dgk = dgt.T
        return layer_out, grad_tok, dgk, g_gate, g_up, g_down

    return jax.shard_map(device_step, mesh=mesh,
                         in_specs=(tok_spec, tok_spec, tok_spec, exp_spec, exp_spec, exp_spec, tok_spec),
                         out_specs=(tok_spec, tok_spec, tok_spec, tok_spec, tok_spec, tok_spec), check_vma=False)
```

```python
import functools

import jax
import jax.numpy as jnp
from jax import lax
from jax.experimental import pallas as pl
from jax.experimental.pallas import tpu as pltpu
from jax.sharding import PartitionSpec as P


F32 = jnp.float32
BF16 = jnp.bfloat16
MESH = pl.DeviceIdType.MESH

TD = 64
D = 2048
F = 1408
K = 6
E = 4
CAP = 24
ND = 8
ROWS = ND * CAP

NT = (((1,), (1,)), ((), ()))
TN = (((0,), (0,)), ((), ()))


def dot(a, b, dims=None):
    if dims is None:
        return jnp.dot(a, b, preferred_element_type=F32)
    return lax.dot_general(a, b, dims, preferred_element_type=F32)


def place():
    y = lax.axis_index('ei')
    o = lax.axis_index('eo')
    x = o // 2
    c = o % 2
    return y, x, c


def flip_if(v, f):
    return v + f - 2 * v * f


def main_kernel(x_hbm, dy_hbm, id_hbm, ga_hbm, wg_hbm, wu_hbm, wd_hbm,
                y_out, dgt_out, s1_out, own_out, sec_out, xs_out, us_out, hs_out, dgu_out,
                wgu, wd, xall, dyall, idall, gaall, rk, gt, psel, ab, oall, py, rb0, rb1, rb2,
                dgs, dgr, xsb, usb, hsb, dgb,
                wsem, lsem, snd, rcv, rs_s, rs_r, dg_s, dg_r, osem, psem, credit):
    dp = lax.axis_index('dp')
    y, x, c = place()
    chip = y * 2 + x
    me = chip * 2 + c
    yp, xp = flip_if(y, c), flip_if(x, 1 - c)
    ys, xs = flip_if(y, 1 - c), flip_if(x, c)
    cp, cs, cd = yp * 2 + xp, ys * 2 + xs, (1 - y) * 2 + (1 - x)

    def dev(yy, xx, cc):
        return (dp, yy, xx * 2 + cc)

    partner, prim, sec = dev(y, x, 1 - c), dev(yp, xp, c), dev(ys, xs, c)

    def rcopy(src, dst, ss, rs, target):
        return pltpu.make_async_remote_copy(src_ref=src, dst_ref=dst, send_sem=ss, recv_sem=rs,
                                            device_id=target, device_id_type=MESH)

    def load(src, dst, sem):
        return pltpu.make_async_copy(src, dst, sem)

    def start_gate_up(e, sl):
        for lo in range(0, D, 256):
            rows = pl.ds(lo, 256)
            load(wg_hbm.at[e, rows], wgu.at[sl, rows, pl.ds(0, F)], wsem.at[sl, 0]).start()
            load(wu_hbm.at[e, rows], wgu.at[sl, rows, pl.ds(F, F)], wsem.at[sl, 1]).start()

    def start_down(e, sl):
        for lo in range(0, F, 176):
            rows = pl.ds(lo, 176)
            load(wd_hbm.at[e, rows], wd.at[sl, rows], wsem.at[sl, 2]).start()

    def wait_gate_up(e, sl):
        load(wg_hbm.at[e], wgu.at[sl, :, pl.ds(0, F)], wsem.at[sl, 0]).wait()
        load(wu_hbm.at[e], wgu.at[sl, :, pl.ds(F, F)], wsem.at[sl, 1]).wait()

    def wait_down(e, sl):
        load(wd_hbm.at[e], wd.at[sl], wsem.at[sl, 2]).wait()

    ins = (load(id_hbm, idall.at[me], lsem.at[0]), load(ga_hbm, gaall.at[me], lsem.at[1]),
           load(x_hbm, xall.at[me], lsem.at[2]), load(dy_hbm, dyall.at[me], lsem.at[3]))
    for cpy in ins:
        cpy.start()

    barrier = pltpu.get_barrier_semaphore()
    others = [lax.rem(me + k, ND) for k in range(1, ND)]
    for t in others:
        pl.semaphore_signal(barrier, inc=1, device_id=(dp, t // 4, lax.rem(t, 4)), device_id_type=MESH)
    pl.semaphore_wait(barrier, ND - 1)

    hw = TD // 2
    bufs = (lambda k: idall.at[k], lambda k: gaall.at[k],
            lambda k: xall.at[k, pl.ds(0, hw)], lambda k: xall.at[k, pl.ds(hw, hw)],
            lambda k: dyall.at[k])
    me_p, me_s, me_d = cp * 2 + c, cs * 2 + c, cd * 2 + c

    def ag_send(st, chunk, k, r, target):
        buf = bufs[st]
        return rcopy(buf(chunk), buf(chunk), snd.at[st, k], rcv.at[st, r], target)

    def ag_wait(st, chunk, r):
        ag_send(st, chunk, 0, r, partner).wait_recv()

    def ag_open(st):
        ag_send(st, me, 0, 0, prim).start()
        ag_send(st, me, 1, 1, sec).start()
        ag_send(st, me, 2, 3, partner).start()

    def ag_first(st):
        ag_wait(st, me_p, 0)
        ag_send(st, me_p, 3, 2, sec).start()
        ag_send(st, me_p, 4, 5, partner).start()

    def ag_second(st):
        ag_wait(st, me_s, 1)
        ag_send(st, me_s, 5, 4, partner).start()

    def ag_diag(st):
        ag_wait(st, me_d, 2)
        ag_send(st, me_d, 6, 6, partner).start()

    def ag_last(st):
        oc = 1 - c
        ag_wait(st, chip * 2 + oc, 3)
        ag_wait(st, cp * 2 + oc, 4)
        ag_wait(st, cs * 2 + oc, 5)
        ag_wait(st, cd * 2 + oc, 6)

    def ag_sent(st):
        for k, (chunk, target) in enumerate(((me, prim), (me, sec), (me, partner), (me_p, sec),
                                             (me_p, partner), (me_s, partner), (me_d, partner))):
            ag_send(st, chunk, k, 0, target).wait_send()

    for st in range(2):
        ins[st].wait()
        ag_open(st)
    ins[2].wait()
    ag_open(2)
    ag_open(3)
    ins[3].wait()
    for e in range(2):
        start_gate_up(e, e)
        start_down(e, e)
    for step in (ag_first, ag_second, ag_diag):
        for st in range(2):
            step(st)
    ag_first(2)
    ag_second(2)
    ag_first(3)
    ag_second(3)
    ag_last(0)
    ag_last(1)

    li = lax.broadcasted_iota(jnp.int32, (128, 128), 0)
    lj = lax.broadcasted_iota(jnp.int32, (128, 128), 1)
    upper = jnp.where((li // TD == lj // TD) & (li < lj), 1.0, 0.0).astype(BF16)
    krow = lax.broadcasted_iota(jnp.int32, (2 * E * CAP, 128), 0).astype(F32)
    pbase = (lax.broadcasted_iota(jnp.int32, (1, 128), 1) // TD * (E * CAP)).astype(F32)
    for p in range(4):
        ids = jnp.concatenate([idall[2 * p], idall[2 * p + 1]], axis=1)
        gv = jnp.concatenate([gaall[2 * p], gaall[2 * p + 1]], axis=1)
        sel = jnp.zeros((2 * E * CAP, 128), F32)
        for e in range(E):
            eq = ids == me * E + e
            hit = jnp.sum(jnp.where(eq, 1.0, 0.0), axis=0, keepdims=True)
            gate = jnp.sum(jnp.where(eq, gv, 0.0), axis=0, keepdims=True)
            hit8 = jnp.broadcast_to(hit, (8, 128))
            rank = jnp.where(hit8 > 0.5, dot(hit8.astype(BF16), upper), -1000.0)
            rk[e, :, 128 * p:128 * (p + 1)] = rank
            gt[e, :, 128 * p:128 * (p + 1)] = jnp.broadcast_to(gate, (8, 128))
            sel = jnp.where(rank[0:1, :] + pbase + float(e * CAP) == krow, 1.0, sel)
        psel[p] = sel.astype(BF16)

    tok = lax.broadcasted_iota(jnp.int32, (1, ND * TD), 1)
    slot_base = (tok // TD * CAP).astype(F32)
    slot_row = lax.broadcasted_iota(jnp.int32, (ROWS, ND * TD), 0).astype(F32)

    def slot_mask(e):
        return (rk[e][0:1, :] + slot_base) == slot_row

    def put_rows(e, c0, width, val):
        for s in range(ND):
            oall[s, e, :, c0:c0 + width] = val[s * CAP:(s + 1) * CAP]

    ag_diag(2)
    ag_diag(3)
    ag_open(4)
    ag_last(2)
    ag_last(3)

    def fwd(e, carry):
        sl = lax.rem(e, 2)
        sel = jnp.where(slot_mask(e), 1.0, 0.0).astype(BF16)

        @pl.when(e > 0)
        def _():
            load(xsb, xs_out.at[e], osem.at[0]).wait()
            load(hsb, hs_out.at[e], osem.at[1]).wait()

        for n in range(4):
            xsb[:, 512 * n:512 * (n + 1)] = dot(sel, xall[:, :, 512 * n:512 * (n + 1)].reshape(ND * TD, 512)).astype(BF16)
        load(xsb, xs_out.at[e], osem.at[0]).start()
        wait_gate_up(e, sl)
        for n in range(6):
            lo, w = 256 * n, 256 if n < 5 else 128
            if w == 256:
                a = dot(xsb[...], wgu[sl, :, lo:lo + w])
                b = dot(xsb[...], wgu[sl, :, F + lo:F + lo + w])
            else:
                rhs = jnp.concatenate([wgu[sl, :, lo:lo + w], wgu[sl, :, F + lo:F + lo + w]], axis=1)
                r = dot(xsb[...], rhs)
                a, b = r[:, :w], r[:, w:]
            ab[e, :, lo:lo + w] = a
            ab[e, :, F + lo:F + lo + w] = b
            hsb[:, lo:lo + w] = (a * jax.nn.sigmoid(a) * b).astype(BF16)
        load(hsb, hs_out.at[e], osem.at[1]).start()

        @pl.when(e < 2)
        def _():
            start_gate_up(e + 2, sl)

        wait_down(e, sl)
        for n in range(8):
            put_rows(e, 256 * n, 256, dot(hsb[...], wd[sl, :, 256 * n:256 * (n + 1)]).astype(BF16))

        @pl.when(e < 2)
        def _():
            start_down(e + 2, sl)

        @pl.when(e == 1)
        def _():
            ag_first(4)

        @pl.when(e == 2)
        def _():
            ag_second(4)
            ag_diag(4)

        return carry

    lax.fori_loop(0, E, fwd, 0)
    load(xsb, xs_out.at[E - 1], osem.at[0]).wait()
    load(hsb, hs_out.at[E - 1], osem.at[1]).wait()
    ag_last(4)

    def combine_y(p, carry):
        lanes = pl.ds(pl.multiple_of(p * 128, 128), 128)
        gates = jnp.zeros((2 * E * CAP, 128), F32)
        for e in range(E):
            hit = rk[e, :, lanes][0:1, :] + pbase + float(e * CAP) == krow
            gates = jnp.where(hit, gt[e, :, lanes][0:1, :], gates)
        g1 = gates.astype(BF16)
        rest = gates - g1.astype(F32)
        g2 = rest.astype(BF16)
        g3 = (rest - g2.astype(F32)).astype(BF16)
        lhs = jnp.concatenate([g1, g2, g3], axis=1)
        for n in range(4):
            cols = slice(512 * n, 512 * (n + 1))
            rhs = oall[pl.ds(2 * p, 2), :, :, cols].reshape(2 * E * CAP, 512)
            r = dot(lhs, rhs, TN)
            r = r[0:128] + (r[128:256] + r[256:384])
            py[0, p, :, cols] = r[0:TD]
            py[1, p, :, cols] = r[TD:]
        return carry

    lax.fori_loop(0, 4, combine_y, 0)

    rs0 = rcopy(py.at[1 - c], rb0, rs_s.at[0], rs_r.at[0], partner)
    rs1a = rcopy(py.at[c, cd], rb1.at[1], rs_s.at[1], rs_r.at[1], prim)
    rs1b = rcopy(py.at[c, cp], rb1.at[0], rs_s.at[2], rs_r.at[2], prim)
    rs2 = rcopy(py.at[c, cs], rb2, rs_s.at[3], rs_r.at[3], sec)
    rs0.start()

    def dx_copy(m):
        cols = pl.ds(512 * m, 512)
        return rcopy(ab.at[:, pl.ds(pl.multiple_of((1 - c) * TD, TD), TD), cols], rb0.at[:, :, cols],
                     rs_s.at[4 + m], rs_r.at[4 + m], partner)

    def combine_dx(m):
        cols = slice(512 * m, 512 * (m + 1))

        def body(p, carry):
            rhs = oall[pl.ds(2 * p, 2), :, :, cols].reshape(2 * E * CAP, 512)
            ab[p, 0:2 * TD, cols] = dot(psel[p], rhs, TN)
            return carry

        lax.fori_loop(0, 4, body, 0)
        dx_copy(m).start()

    def bwd(n, carry):
        e = E - 1 - n
        sl = lax.rem(e, 2)
        mask = slot_mask(e)
        sel = jnp.where(mask, 1.0, 0.0).astype(BF16)
        gcol = jnp.sum(jnp.where(mask, gt[e][0:1, :], 0.0), axis=1, keepdims=True)

        @pl.when(n > 0)
        def _():
            load(usb, us_out.at[e], osem.at[0]).wait()
            load(dgb, dgu_out.at[e], osem.at[1]).wait()

        dgv = jnp.zeros((ROWS, 1), F32)
        for m in range(4):
            c0 = 512 * m
            dye = dot(sel, dyall[:, :, c0:c0 + 512].reshape(ND * TD, 512))
            usb[:, c0:c0 + 512] = (gcol * dye).astype(BF16)
            oe = jnp.concatenate([oall[s, e, :, c0:c0 + 512] for s in range(ND)], axis=0).astype(F32)
            dgv = dgv + jnp.sum(dye * oe, axis=1, keepdims=True)
        dgrow = jnp.sum(jnp.where(mask, dgv, 0.0), axis=0, keepdims=True)
        dgs[e] = jnp.broadcast_to(dgrow, (8, ND * TD))
        load(usb, us_out.at[e], osem.at[0]).start()

        @pl.when(n >= 2)
        def _():
            wait_down(e, sl)

        for lo in range(0, F, 256):
            hi = min(lo + 256, F)
            q = dot(wd[sl, lo:hi, :], usb[...], NT).T
            a = ab[e, :, lo:hi]
            b = ab[e, :, F + lo:F + hi]
            s = jax.nn.sigmoid(a)
            dgb[:, F + lo:F + hi] = (q * a * s).astype(BF16)
            dgb[:, lo:hi] = (q * b * s * (1.0 + a * (1.0 - s))).astype(BF16)
        load(dgb, dgu_out.at[e], osem.at[1]).start()

        @pl.when(n < 2)
        def _():
            start_down(1 - n, sl)

        @pl.when(n == 2)
        def _():
            rs1a.wait_recv()
            py[c, cs] = py[c, cs] + rb1[1]
            rs2.start()

        @pl.when(n >= 2)
        def _():
            wait_gate_up(e, sl)

        for m in range(4):
            dxt = dot(wgu[sl, 512 * m:512 * (m + 1), :], dgb[...], NT)
            put_rows(e, 512 * m, 512, dxt.T.astype(BF16))

        @pl.when(n < 2)
        def _():
            start_gate_up(1 - n, sl)

        @pl.when(n == 0)
        def _():
            rs0.wait()
            py[c] = py[c] + rb0[...]
            rs1a.start()
            rs1b.start()
            pl.semaphore_signal(credit, inc=1, device_id=partner, device_id_type=MESH)

        return carry

    lax.fori_loop(0, E, bwd, 0)
    pl.semaphore_wait(credit, 1)
    for m in range(4):
        combine_dx(m)
    load(usb, us_out.at[0], osem.at[0]).wait()
    load(dgb, dgu_out.at[0], osem.at[1]).wait()

    sends = []
    for i, t in enumerate(others):
        lanes = pl.ds(pl.multiple_of(t // 2 * 128, 128), 128)
        cpy = rcopy(dgs.at[:, :, lanes], dgr.at[me], dg_s.at[i], dg_r.at[me],
                    (dp, t // 4, lax.rem(t, 4)))
        cpy.start()
        sends.append(cpy)
    dgr[me] = dgs[:, :, pl.ds(pl.multiple_of(chip * 128, 128), 128)]

    rs1b.wait_recv()
    rs2.wait_recv()
    y_out[...] = (py[c, chip] + rb1[0] + rb2[...]).astype(BF16)

    own_rows = pl.ds(pl.multiple_of(c * TD, TD), TD)
    dst = ((cp, s1_out.at[0]), (cd, s1_out.at[1]), (chip, own_out), (cs, sec_out))
    parts = []
    for m in range(4):
        dx_copy(m).wait_recv()
        for i, (k, out) in enumerate(dst):
            cols = slice(512 * m, 512 * (m + 1))
            ab[i, 2 * TD:3 * TD, cols] = ab[k, own_rows, cols] + rb0[k, :, cols]
            cpy = load(ab.at[i, pl.ds(2 * TD, TD), pl.ds(512 * m, 512)], out.at[:, pl.ds(512 * m, 512)], psem.at[i, m])
            cpy.start()
            parts.append(cpy)

    for i, t in enumerate(others):
        rcopy(dgs.at[:, :, pl.ds(0, 128)], dgr.at[t], dg_s.at[i], dg_r.at[t], partner).wait_recv()
    ids = idall[me]
    acc = jnp.zeros((K, TD), F32)
    for t in range(ND):
        for e in range(E):
            row = dgr[t, e][0:1, :]
            row = jnp.where(c == 0, row[:, 0:TD], row[:, TD:2 * TD])
            acc = acc + jnp.where(ids == t * E + e, row, 0.0)
    dgt_out[...] = acc

    for m in range(4):
        dx_copy(m).wait_send()
    rs1a.wait_send()
    rs1b.wait_send()
    rs2.wait_send()
    for st in range(5):
        ag_sent(st)
    for cpy in sends:
        cpy.wait_send()
    for cpy in parts:
        cpy.wait()


def run_main(tok, dy, idt, gat, wg, wu, wd):
    anys = pl.BlockSpec(memory_space=pl.ANY)
    vm = pl.BlockSpec(memory_space=pltpu.VMEM)
    V = pltpu.VMEM
    S = pltpu.SemaphoreType.DMA
    flops = 2 * E * ROWS * D * F * 6
    return pl.pallas_call(
        main_kernel,
        name='moe_main',
        out_shape=(jax.ShapeDtypeStruct((TD, D), BF16), jax.ShapeDtypeStruct((K, TD), F32),
                   jax.ShapeDtypeStruct((2, TD, D), F32), jax.ShapeDtypeStruct((TD, D), F32),
                   jax.ShapeDtypeStruct((TD, D), F32),
                   jax.ShapeDtypeStruct((E, ROWS, D), BF16), jax.ShapeDtypeStruct((E, ROWS, D), BF16),
                   jax.ShapeDtypeStruct((E, ROWS, F), BF16), jax.ShapeDtypeStruct((E, ROWS, 2 * F), BF16)),
        in_specs=[anys] * 7,
        out_specs=(vm, vm) + (anys,) * 7,
        scratch_shapes=[
            V((2, D, 2 * F), BF16), V((2, F, D), BF16),
            V((ND, TD, D), BF16), V((ND, TD, D), BF16), V((ND, K, TD), jnp.int32), V((ND, K, TD), F32),
            V((E, 8, ND * TD), F32), V((E, 8, ND * TD), F32), V((4, 2 * E * CAP, 128), BF16),
            V((E, ROWS, 2 * F), F32), V((ND, E, CAP, D), BF16),
            V((2, 4, TD, D), F32), V((4, TD, D), F32), V((2, TD, D), F32), V((TD, D), F32),
            V((E, 8, ND * TD), F32), V((ND, E, 8, 128), F32),
            V((ROWS, D), BF16), V((ROWS, D), BF16), V((ROWS, F), BF16), V((ROWS, 2 * F), BF16),
            S((2, 3)), S((4,)), S((5, 7)), S((5, 7)), S((8,)), S((8,)), S((7,)), S((ND,)), S((2,)), S((4, 4)),
            pltpu.SemaphoreType.REGULAR,
        ],
        compiler_params=pltpu.CompilerParams(collective_id=0, has_side_effects=True,
                                             vmem_limit_bytes=67043328),
        cost_estimate=pl.CostEstimate(flops=flops, bytes_accessed=120_000_000, transcendentals=0),
    )(tok, dy, idt, gat, wg, wu, wd)


RING = 4


def ring_loop(steps, ring, outs, compute):
    def body(i, carry):
        slot = lax.rem(i, ring)

        @pl.when(i >= ring)
        def _():
            for cpy in outs(i - ring, slot):
                cpy.wait()

        compute(i, slot)
        for cpy in outs(i, slot):
            cpy.start()
        return carry

    lax.fori_loop(0, steps, body, 0)
    for k in range(ring):
        i = steps - ring + k
        for cpy in outs(i, i % ring):
            cpy.wait()


def gate_up_kernel(x_hbm, g_hbm, y_hbm, dg_hbm, og_hbm, ou_hbm, oy_hbm, odg_hbm,
                   x_v, g_v, og_v, ou_v, y_v, dg_v, isem, osem, psem):
    through = ((y_hbm, y_v, oy_hbm), (dg_hbm, dg_v, odg_hbm))

    def ins(e):
        return (pltpu.make_async_copy(x_hbm.at[e], x_v.at[e], isem.at[e, 0]),
                pltpu.make_async_copy(g_hbm.at[e], g_v.at[e], isem.at[e, 1]))

    for e in range(E):
        for cpy in ins(e):
            cpy.start()

    def outs(i, slot):
        rows = pl.ds(pl.multiple_of(lax.rem(i, 4) * 512, 512), 512)
        return (pltpu.make_async_copy(og_v.at[slot], og_hbm.at[i // 4, rows], osem.at[slot, 0]),
                pltpu.make_async_copy(ou_v.at[slot], ou_hbm.at[i // 4, rows], osem.at[slot, 1]))

    def compute(i, slot):
        e = i // 4

        @pl.when(lax.rem(i, 4) == 0)
        def _():
            for cpy in ins(e):
                cpy.wait()

        @pl.when(i == 4)
        def _():
            for k, (src, mid, _) in enumerate(through):
                pltpu.make_async_copy(src, mid, psem.at[k, 0]).start()

        @pl.when(i == 8)
        def _():
            for k, (src, mid, dst) in enumerate(through):
                pltpu.make_async_copy(src, mid, psem.at[k, 0]).wait()
                pltpu.make_async_copy(mid, dst, psem.at[k, 1]).start()

        cols = pl.ds(pl.multiple_of(lax.rem(i, 4) * 512, 512), 512)
        r = dot(x_v[e, :, cols], g_v[e], TN)
        og_v[slot] = r[:, :F].astype(BF16)
        ou_v[slot] = r[:, F:].astype(BF16)

    ring_loop(4 * E, RING, outs, compute)
    for k, (_, mid, dst) in enumerate(through):
        pltpu.make_async_copy(mid, dst, psem.at[k, 1]).wait()


def run_gate_up(xs, dgu, y, dgt):
    anys = pl.BlockSpec(memory_space=pl.ANY)
    V = pltpu.VMEM
    return pl.pallas_call(
        gate_up_kernel, name='moe_dw_gate_up',
        in_specs=[anys] * 4, out_specs=(anys,) * 4,
        out_shape=(jax.ShapeDtypeStruct((E, D, F), BF16),) * 2
        + (jax.ShapeDtypeStruct((TD, D), BF16), jax.ShapeDtypeStruct((K, TD), F32)),
        scratch_shapes=[V((E, ROWS, D), BF16), V((E, ROWS, 2 * F), BF16),
                        V((RING, 512, F), BF16), V((RING, 512, F), BF16), V((TD, D), BF16), V((K, TD), F32),
                        pltpu.SemaphoreType.DMA((E, 2)), pltpu.SemaphoreType.DMA((RING, 2)),
                        pltpu.SemaphoreType.DMA((2, 2))],
        compiler_params=pltpu.CompilerParams(vmem_limit_bytes=67043328),
        cost_estimate=pl.CostEstimate(flops=4 * E * ROWS * D * F, bytes_accessed=55_000_000, transcendentals=0),
    )(xs, dgu, y, dgt)


def down_kernel(h_hbm, u_hbm, o_hbm, h_v, u_v, ht_v, o_v, isem, osem):
    def ins(e):
        return (pltpu.make_async_copy(h_hbm.at[e], h_v.at[e], isem.at[e, 0]),
                pltpu.make_async_copy(u_hbm.at[e], u_v.at[e], isem.at[e, 1]))

    for e in range(E):
        for cpy in ins(e):
            cpy.start()

    def cols(i):
        return pl.ds(pl.multiple_of(lax.rem(i, 2) * 1024, 1024), 1024)

    def outs(i, slot):
        halves = []
        for k in range(2):
            rows = pl.ds(704 * k, 704)
            halves.append(pltpu.make_async_copy(o_v.at[slot, rows], o_hbm.at[i // 2, rows, cols(i)], osem.at[slot, k]))
        return halves

    def compute(i, slot):
        e = i // 2

        @pl.when(lax.rem(i, 2) == 0)
        def _():
            for cpy in ins(e):
                cpy.wait()
            ht_v[...] = h_v[e].T

        o_v[slot] = dot(ht_v[...], u_v[e, :, cols(i)]).astype(BF16)

    ring_loop(2 * E, RING, outs, compute)


def run_down(hs, us):
    anys = pl.BlockSpec(memory_space=pl.ANY)
    V = pltpu.VMEM
    return pl.pallas_call(
        down_kernel, name='moe_dw_down',
        in_specs=[anys, anys], out_specs=anys,
        out_shape=jax.ShapeDtypeStruct((E, F, D), BF16),
        scratch_shapes=[V((E, ROWS, F), BF16), V((E, ROWS, D), BF16), V((F, ROWS), BF16), V((RING, F, 1024), BF16),
                        pltpu.SemaphoreType.DMA((E, 2)), pltpu.SemaphoreType.DMA((RING, 2))],
        compiler_params=pltpu.CompilerParams(vmem_limit_bytes=67043328),
        cost_estimate=pl.CostEstimate(flops=2 * E * ROWS * D * F, bytes_accessed=28_000_000, transcendentals=0),
    )(hs, us)


def exchange_pairs(kind):
    pairs = []
    for y in range(2):
        for x in range(2):
            for c in range(2):
                if (kind == 'prim') == (c == 0):
                    t = (y, 1 - x, c)
                else:
                    t = (1 - y, x, c)
                pairs.append((y * 4 + x * 2 + c, t[0] * 4 + t[1] * 2 + t[2]))
    return pairs


def solution(mesh):
    tok_spec = P(('dp', 'ei', 'eo'))
    exp_spec = P(('ei', 'eo'))

    def device_step(tok, idx, gate, wg, wu, wd, dy):
        layer_out, dgt, s1, own, second, xs, us, hs, dgu = run_main(tok, dy, idx.T, gate.T, wg, wu, wd)
        perm = functools.partial(lax.ppermute, axis_name=('ei', 'eo'))
        r1 = perm(s1, perm=exchange_pairs('prim'))
        g_gate, g_up, layer_out, dgt = run_gate_up(xs, dgu, layer_out, dgt)
        g_down = run_down(hs, us)
        r2 = perm(second + r1[1], perm=exchange_pairs('sec'))
        grad_tok = (own + r1[0] + r2).astype(BF16)
        dgk = dgt.T
        return layer_out, grad_tok, dgk, g_gate, g_up, g_down

    return jax.shard_map(device_step, mesh=mesh,
                         in_specs=(tok_spec, tok_spec, tok_spec, exp_spec, exp_spec, exp_spec, tok_spec),
                         out_specs=(tok_spec, tok_spec, tok_spec, tok_spec, tok_spec, tok_spec), check_vma=False)
```
